32 devices in a mesh: pair: 4 (over y, x), value: 8 (over z, core).
Axes of the slice: x: 2, y: 2, z: 4, core: 2. Of those that a mesh axis runs over, the one named last changes fastest.
Arguments:
- student: bfloat16 [1536, 65536], P('pair', 'value'), may hold values from -8 to 8
- teacher: bfloat16 [1536, 65536], P('pair', 'value'), may hold values from -8 to 8
- bw_table: float32 [8], replicated, may hold values from 0.5 to 8
- bw_index: int32 [4], replicated, may hold values from 0 to 7
- group_ids: int32 [1536], replicated, may hold values from 0 to 15, as said below
Outputs:
- force: float32 [1536, 65536], P('pair', 'value')
- loss: float32 [], replicated
The draws below stay inside these ranges and needn't reach their ends.
Inputs may be any that keep to these rules, and one draw needn't show every extreme that they name: `group_ids`: every group from 0 to 15 holds at least one sample.
All inputs are finite; a program needn't handle non-finite values.
Results may differ from the reference program's by a relative error of at most 0.00045.
The reference program's roundings to bfloat16 on the way count: a program that leaves them out, or rounds other values in their place, can miss the bound.
Values may be sent and summed in bfloat16 or wider, within the bound.
No kernel may reach another device: no remote copies, remote signals or barrier semaphores. Data moves between devices by JAX's collectives and lax.ppermute only.
A program may use at most 128 MiB of HBM per device.

```python
import math
import jax
import jax.numpy as jnp
from jax import lax

LATENT = 65536
NBW = 8
NSEL = 4
GROUPS = 16
SAMPLES = 1536


def group_draw(key):
    key_base, key_shuffle = jax.random.split(jax.random.fold_in(key, 7))
    groups = jax.random.randint(key_base, (SAMPLES,), 0, GROUPS, dtype=jnp.int32)
    shuffle = jax.random.permutation(key_shuffle, SAMPLES)
    return groups.at[shuffle[:GROUPS]].set(jnp.arange(GROUPS, dtype=jnp.int32))


def latent_pair(key):
    groups = group_draw(key)
    subkeys = jax.random.split(jax.random.fold_in(key, 31), 7)
    pattern_count = 32
    member = (groups[:, None] == jnp.arange(GROUPS, dtype=jnp.int32)[None, :]).astype(jnp.float32)
    coeffs = jax.random.normal(subkeys[0], (SAMPLES, pattern_count), jnp.float32) * (0.6 / math.sqrt(pattern_count))
    teacher_gaps = jnp.exp(jax.random.uniform(subkeys[1], (SAMPLES, 1), jnp.float32, math.log(0.2), math.log(0.8)))
    centers = 0.8 * jnp.clip(jax.random.normal(subkeys[2], (GROUPS, LATENT), jnp.float32), -4.0, 4.0)
    patterns = jnp.clip(jax.random.normal(subkeys[3], (pattern_count, LATENT), jnp.float32), -4.0, 4.0)
    sample_noise = 0.6 * jnp.clip(jax.random.normal(subkeys[4], (SAMPLES, LATENT), jnp.float32), -4.0, 4.0)
    scales = jnp.exp(jax.random.uniform(subkeys[5], (SAMPLES, 1), jnp.float32, math.log(0.5), math.log(1.0)))
    shifts = jnp.clip(jax.random.normal(subkeys[6], (SAMPLES, LATENT), jnp.float32), -4.0, 4.0)
    student = jnp.dot(member, centers, precision=lax.Precision.HIGHEST)
    student = student + jnp.dot(coeffs, patterns, precision=lax.Precision.HIGHEST)
    student = student + sample_noise * scales
    teacher = student + shifts * teacher_gaps
    student = jnp.clip(student, -8.0, 8.0).astype(jnp.bfloat16)
    teacher = jnp.clip(teacher, -8.0, 8.0).astype(jnp.bfloat16)
    return (student, teacher)


def draw_student(key, part):
    return latent_pair(key)[0]


def draw_teacher(key, part):
    return latent_pair(key)[1]


def draw_group_ids(key, part):
    return group_draw(key)


def with_ends(drawn, stream_key, least, largest):
    longest = drawn.shape.index(max(drawn.shape))
    spots = []
    for shift in (0, 1):
        where = [jax.random.randint(jax.random.fold_in(stream_key, axis), (), 0, length) for axis, length in enumerate(drawn.shape)]
        where[longest] = (where[longest] + shift) % drawn.shape[longest]
        spots.append(tuple(where))
    return drawn.at[spots[0]].set(least).at[spots[1]].set(largest)


def setup_inputs(seed: int = 0) -> dict:
    seeds = jax.random.split(jax.random.key(seed), 6)
    student = draw_student(jax.random.fold_in(seeds[5], 71), 0)
    teacher = draw_teacher(jax.random.fold_in(seeds[5], 71), 0)
    bw_table = jnp.clip(jnp.exp(jax.random.uniform(seeds[2], (NBW,), jnp.float32, math.log(0.5), math.log(8.0))), 0.5, 8.0)
    bw_index = with_ends(jax.random.randint(seeds[3], (NSEL,), 0, NBW), jax.random.fold_in(seeds[3], 1), 0, NBW - 1).astype(jnp.int32)
    group_ids = draw_group_ids(jax.random.fold_in(seeds[5], 71), 0)
    return {"student": student, "teacher": teacher, "bw_table": bw_table, "bw_index": bw_index, "group_ids": group_ids}


def kernel_terms(gram_self, gram_cross, norm_rows, norm_student, norm_teacher, same_group, heights, latent):
    dist_self = jnp.maximum(norm_rows[:, None] + norm_student[None, :] - 2.0 * gram_self, 0.0)
    dist_cross = jnp.maximum(norm_rows[:, None] + norm_teacher[None, :] - 2.0 * gram_cross, 0.0)
    kern_self = jnp.zeros_like(dist_self)
    kern_cross = jnp.zeros_like(dist_cross)
    weight_self = jnp.zeros_like(dist_self)
    weight_cross = jnp.zeros_like(dist_cross)
    count = heights.shape[0]
    for member in range(count):
        height = heights[member]
        width_now = height * latent
        exp_self = jnp.exp(-dist_self / width_now)
        exp_cross = jnp.exp(-dist_cross / width_now)
        kern_self = kern_self + exp_self
        kern_cross = kern_cross + exp_cross
        weight_self = weight_self + exp_self / height
        weight_cross = weight_cross + exp_cross / height
    kern_self = kern_self / count * same_group
    kern_cross = kern_cross / count * same_group
    weight_self = weight_self / count * same_group
    weight_cross = weight_cross / count * same_group
    row_loss = jnp.sum(kern_self - 2.0 * kern_cross, axis=1)
    total_self = jnp.sum(weight_self, axis=1)
    total_cross = jnp.sum(weight_cross, axis=1)
    return weight_self.astype(jnp.bfloat16), weight_cross.astype(jnp.bfloat16), row_loss, total_self, total_cross


def reference(student, teacher, bw_table, bw_index, group_ids):
    student_wide = student.astype(jnp.float32)
    teacher_wide = teacher.astype(jnp.float32)
    norm_student = jnp.sum(student_wide * student_wide, axis=1)
    norm_teacher = jnp.sum(teacher_wide * teacher_wide, axis=1)
    gram_self = jnp.dot(student, student.T, preferred_element_type=jnp.float32)
    gram_cross = jnp.dot(student, teacher.T, preferred_element_type=jnp.float32)
    heights = bw_table[bw_index]
    same_group = (group_ids[:, None] == group_ids[None, :]).astype(jnp.float32)
    group_sizes = jnp.sum(same_group, axis=1)
    weight_self, weight_cross, row_loss, total_self, total_cross = kernel_terms(
        gram_self, gram_cross, norm_student, norm_student, norm_teacher, same_group, heights, float(LATENT))
    loss = jnp.sum(row_loss / group_sizes) / SAMPLES
    pulled = student_wide * (total_cross - total_self)[:, None]
    pulled = pulled + jnp.dot(weight_self, student, preferred_element_type=jnp.float32)
    pulled = pulled - jnp.dot(weight_cross, teacher, preferred_element_type=jnp.float32)
    force = pulled / group_sizes[:, None]
    return force, loss
```

```python
import functools

import jax
import jax.numpy as jnp
from jax import lax
from jax.experimental import pallas as pl
from jax.experimental.pallas import tpu as pltpu
from jax.sharding import PartitionSpec as P

GROUPS = 16
SLOTS = 128
ROWS = 512
PAD = 16
HALF_TOP = 32768.0
CHUNKS = 4


def kernel_terms(
    gram_self, gram_cross, norm_rows, norm_student, norm_teacher, same_group, heights, latent
):
    dist_self = jnp.maximum(norm_rows[..., :, None] + norm_student[..., None, :] - 2.0 * gram_self, 0.0)
    dist_cross = jnp.maximum(norm_rows[..., :, None] + norm_teacher[..., None, :] - 2.0 * gram_cross, 0.0)
    kern_self = jnp.zeros_like(dist_self)
    kern_cross = jnp.zeros_like(dist_cross)
    weight_self = jnp.zeros_like(dist_self)
    weight_cross = jnp.zeros_like(dist_cross)
    count = heights.shape[0]
    for member in range(count):
        height = heights[member]
        width_now = height * latent
        exp_self = jnp.exp(-dist_self / width_now)
        exp_cross = jnp.exp(-dist_cross / width_now)
        kern_self = kern_self + exp_self
        kern_cross = kern_cross + exp_cross
        weight_self = weight_self + exp_self / height
        weight_cross = weight_cross + exp_cross / height
    kern_self = kern_self / count * same_group
    kern_cross = kern_cross / count * same_group
    weight_self = weight_self / count * same_group
    weight_cross = weight_cross / count * same_group
    row_loss = jnp.sum(kern_self - 2.0 * kern_cross, axis=-1)
    total_self = jnp.sum(weight_self, axis=-1)
    total_cross = jnp.sum(weight_cross, axis=-1)
    return (
        weight_self.astype(jnp.bfloat16),
        weight_cross.astype(jnp.bfloat16),
        row_loss,
        total_self,
        total_cross,
    )


def pick_heights(bw_table, bw_index):
    table_slots = jnp.arange(bw_table.shape[0], dtype=jnp.int32)
    return jnp.sum(
        jnp.where(bw_index[:, None] == table_slots[None, :], bw_table[None, :], 0.0), axis=1
    )


def swap(x, axis, bits):
    count = lax.axis_size(axis)
    return lax.ppermute(x, axis, [(i, i ^ bits) for i in range(count)])


def take(x, index):
    return lax.dynamic_index_in_dim(x, index, 0, keepdims=False)


def placed(parts, me):
    x = jnp.stack(parts)
    bit = 1
    while bit < len(parts):
        order = [i ^ bit for i in range(len(parts))]
        x = jnp.where((me & bit) != 0, jnp.stack([x[i] for i in order]), x)
        bit *= 2
    return x


def reduce_stages():
    values = lax.axis_size("value")
    value = lax.axis_index("value")
    pair = lax.axis_index("pair")
    stages = [("value", 1, min(values, 2), value & 1)]
    stages.append(("pair", 1, lax.axis_size("pair"), pair))
    if values >= 8:
        stages.append(("value", 2, 4, (value >> 1) & 3))
        done = 8
    else:
        done = 2
    rest = []
    while done < values:
        rest.append(done)
        done *= 2
    return stages, rest


def all_sum(x):
    stages, rest = reduce_stages()
    for axis, unit, ways, me in stages:
        x = x.reshape((ways, x.shape[0] // ways) + x.shape[1:])
        got = [swap(take(x, me ^ k), axis, unit * k) for k in range(1, ways)]
        x = sum(got, take(x, me))
    for bits in rest:
        x = x + swap(x, "value", bits)
    for axis, unit, ways, me in reversed(stages):
        got = [x] + [swap(x, axis, unit * k) for k in range(1, ways)]
        x = placed(got, me)
        x = x.reshape((x.shape[0] * x.shape[1],) + x.shape[2:])
    return x


def pieces_of(x, pair, ways, lo, size):
    part = x.shape[1] // ways
    return [lax.dynamic_slice_in_dim(x, (pair ^ k) * part + lo, size, 1) for k in range(ways)]


def exchange(x, pair, ways, lo, size, order):
    pieces = pieces_of(x, pair, ways, lo, size)
    got = {0: pieces[0]}
    for k in order:
        got[k] = swap(pieces[k], "pair", k)
    return [got[k] for k in range(ways)]


def general(student, teacher, bw_table, bw_index, group_ids):
    ways = lax.axis_size("pair")
    pair = lax.axis_index("pair")
    rows, width = student.shape
    part = width // ways
    samples = rows * ways
    latent = float(width * lax.axis_size("value"))
    order = list(range(1, ways))
    block = SLOTS

    def gathered(x):
        full = jnp.zeros((samples, part), x.dtype)
        for k, got in enumerate(exchange(x, pair, ways, 0, part, order)):
            full = lax.dynamic_update_slice_in_dim(full, got, (pair ^ k) * rows, 0)
        return full

    def lane_sum(x):
        flat = x.reshape(-1, SLOTS)
        padded = jnp.pad(flat, ((0, -flat.shape[0] % 256), (0, 0)))
        return all_sum(padded)[: flat.shape[0]].reshape(x.shape)

    student_all, teacher_all = gathered(student), gathered(teacher)
    norms = jnp.stack([jnp.sum(x.astype(jnp.float32) ** 2, axis=1) for x in (student_all, teacher_all)])
    norm_student, norm_teacher = lane_sum(norms)
    heights = pick_heights(bw_table, bw_index)
    dims = (((1,), (1,)), ((), ()))

    def step(b, state):
        force, loss = state
        own = lax.dynamic_slice_in_dim(student_all, b * block, block)
        grams = [
            lax.dot_general(own, x, dims, preferred_element_type=jnp.float32) for x in (student_all, teacher_all)
        ]
        gram_self, gram_cross = lane_sum(jnp.stack(grams))
        own_ids = lax.dynamic_slice_in_dim(group_ids, b * block, block)
        same_group = (own_ids[:, None] == group_ids[None, :]).astype(jnp.float32)
        group_sizes = jnp.sum(same_group, axis=1)
        norm_rows = lax.dynamic_slice_in_dim(norm_student, b * block, block)
        weight_self, weight_cross, row_loss, total_self, total_cross = kernel_terms(
            gram_self, gram_cross, norm_rows, norm_student, norm_teacher, same_group, heights, latent
        )
        pulled = own.astype(jnp.float32) * (total_cross - total_self)[:, None]
        pulled = pulled + jnp.dot(weight_self, student_all, preferred_element_type=jnp.float32)
        pulled = pulled - jnp.dot(weight_cross, teacher_all, preferred_element_type=jnp.float32)
        pulled = pulled / group_sizes[:, None]
        force = lax.dynamic_update_slice_in_dim(force, pulled, b * block, 0)
        return force, loss + jnp.sum(row_loss / group_sizes)

    start = (jnp.zeros((samples, part), jnp.float32), jnp.zeros((), jnp.float32))
    force, loss = lax.fori_loop(0, samples // block, step, start)
    force = force.reshape(ways, rows, part)
    out = jnp.zeros((rows, width), jnp.float32)
    for k in range(ways):
        sent = take(force, pair ^ k)
        sent = swap(sent, "pair", k) if k else sent
        out = lax.dynamic_update_slice_in_dim(out, sent, (pair ^ k) * part, 1)
    return (out, loss / samples)


def slot_kernel(ways, first, *refs):
    pick, refs = refs[0], refs[1:]
    blocks, refs = refs[:ways], refs[ways:]
    slots_out, held = refs if first else refs[1:]
    rows = blocks[0].shape[0]

    @pl.when(pl.program_id(0) == 0)
    def _():
        for k in range(ways):
            held[k * rows : (k + 1) * rows] = blocks[k][...]

    slots_out[...] = jnp.dot(pick[...], held[...], preferred_element_type=jnp.float32).astype(jnp.bfloat16)


def to_slots(pick, blocks, carry, chunk, chunks, part):
    ways = len(blocks)
    rows, size = blocks[0].shape
    slots = pick.shape[0]
    first = carry is None
    in_specs = [pl.BlockSpec((ROWS, ways * rows), lambda i: (i, 0))]
    in_specs += [pl.BlockSpec((rows, size), lambda i: (0, 0))] * ways
    args = [pick, *blocks]
    aliases = {}
    if not first:
        in_specs.append(pl.BlockSpec(memory_space=pl.ANY))
        aliases = {len(args): 0}
        args.append(carry)
    return pl.pallas_call(
        functools.partial(slot_kernel, ways, first),
        grid=(slots // ROWS,),
        in_specs=in_specs,
        out_specs=pl.BlockSpec((ROWS, size), lambda i: (i, chunk)),
        out_shape=jax.ShapeDtypeStruct((slots, part), jnp.bfloat16),
        scratch_shapes=[pltpu.VMEM((ways * rows, size), jnp.bfloat16)],
        input_output_aliases=aliases,
        cost_estimate=pl.CostEstimate(
            flops=2 * slots * size * ways * rows, bytes_accessed=slots * ways * rows * 2, transcendentals=0
        ),
        name="slots",
    )(*args)


def weight_kernel(latent, counts, index, table, self_ref, cross_ref, out, loss):
    step = pl.program_id(0)
    row = lax.broadcasted_iota(jnp.int32, (SLOTS, SLOTS), 0)
    col = lax.broadcasted_iota(jnp.int32, (SLOTS, SLOTS), 1)
    members = index.shape[0]
    scale = [-1.0 / (table[index[m]] * latent) for m in range(members)]
    inverse = [1.0 / (table[index[m]] * members) for m in range(members)]

    @pl.when(step == 0)
    def _():
        loss[...] = jnp.zeros_like(loss)

    for g in range(self_ref.shape[0]):
        size = counts[step * self_ref.shape[0] + g]
        used = (row < size) & (col < size)
        gram_self = self_ref[g]
        diag = jnp.where(row == col, gram_self, 0.0)
        norm_col = jnp.sum(diag, axis=0, keepdims=True)
        norm_row = jnp.sum(diag, axis=1, keepdims=True)

        def terms(gram, norm):
            both = norm_row + norm
            dist = jnp.maximum(both - 2.0 * gram, 0.0)
            kern = jnp.zeros_like(dist)
            weight = jnp.zeros_like(dist)
            for m in range(members):
                e = jnp.exp(dist * scale[m])
                kern = kern + e
                weight = weight + e * inverse[m]
            kern = jnp.where(used, kern, 0.0)
            weight = jnp.where(used, weight, 0.0)
            span = dist + both * (2.0 ** -10) + 1e-30
            return kern, weight, weight * (span * lax.rsqrt(span))

        kern_s, weight_s, reach_s = terms(gram_self, norm_col)
        kern_c, weight_c, reach_c = terms(cross_ref[g, :SLOTS], cross_ref[g, SLOTS : SLOTS + 1])
        count = jnp.maximum(size, 1).astype(jnp.float32)
        pull = jnp.sum(weight_c - weight_s, axis=1, keepdims=True)
        reach = jnp.sum(reach_s + reach_c, axis=1, keepdims=True) * (1.01 / count)
        reach = jnp.maximum(reach, 1e-30).astype(jnp.bfloat16).astype(jnp.float32)
        high = pull.astype(jnp.bfloat16).astype(jnp.float32)
        mid = (pull - high).astype(jnp.bfloat16).astype(jnp.float32)
        low = pull - high - mid
        extra = jnp.where(col == 0, high, jnp.where(col == 1, mid, jnp.where(col == 2, low, 0.0)))
        extra = jnp.where(col == 3, count, jnp.where(col == 4, reach, extra))
        at = slice(g * SLOTS, (g + 1) * SLOTS)
        out[at, :SLOTS] = weight_s.astype(jnp.bfloat16)
        out[at, SLOTS : 2 * SLOTS] = (-weight_c).astype(jnp.bfloat16)
        out[at, 2 * SLOTS :] = extra.astype(jnp.bfloat16)
        part = jnp.sum(kern_s - 2.0 * kern_c, axis=0, keepdims=True) * (1.0 / (count * members))
        loss[...] += jnp.broadcast_to(part, loss.shape)


def weights_of(gram_self, cross, counts, bw_table, bw_index, latent):
    smem = pl.BlockSpec(memory_space=pltpu.SMEM)
    high = cross.shape[1]
    held = 4
    return pl.pallas_call(
        functools.partial(weight_kernel, latent),
        grid=(GROUPS // held,),
        in_specs=[
            smem,
            smem,
            smem,
            pl.BlockSpec((held, SLOTS, SLOTS), lambda g: (g, 0, 0)),
            pl.BlockSpec((held, high, SLOTS), lambda g: (g, 0, 0)),
        ],
        out_specs=[
            pl.BlockSpec((held * SLOTS, 3 * SLOTS), lambda g: (g, 0)),
            pl.BlockSpec((8, SLOTS), lambda g: (0, 0)),
        ],
        out_shape=[
            jax.ShapeDtypeStruct((GROUPS * SLOTS, 3 * SLOTS), jnp.bfloat16),
            jax.ShapeDtypeStruct((8, SLOTS), jnp.float32),
        ],
        cost_estimate=pl.CostEstimate(flops=GROUPS * SLOTS * SLOTS * 60, bytes_accessed=4 << 20, transcendentals=0),
        name="weights",
    )(counts, bw_index, bw_table, gram_self, cross)


def force_kernel(own, spot, put, own_rows, weights, s_slots, t_slots, *refs):
    if own:
        out, reach_out, w_s, w_c, pull, scale = refs
    else:
        out, w_s, w_c, pull, scale = refs
    rows, slots = put.shape

    @pl.when(pl.program_id(0) == 0)
    def _():
        extra = jnp.zeros((rows, SLOTS), jnp.float32)
        for g in range(slots // SLOTS):
            at = slice(g * SLOTS, (g + 1) * SLOTS)
            found = jnp.dot(put[:, at], weights[at], preferred_element_type=jnp.float32)
            w_s[:, at] = found[:, :SLOTS].astype(jnp.bfloat16)
            w_c[:, at] = found[:, SLOTS : 2 * SLOTS].astype(jnp.bfloat16)
            extra = extra + found[:, 2 * SLOTS :]
        pull[...] = extra[:, 0:1] + extra[:, 1:2] + extra[:, 2:3]
        size = extra[:, 3:4]
        reach = extra[:, 4:5]
        if own:
            scale[...] = 1.0 / size
            reach_out[...] = jnp.broadcast_to(reach * (1.0 / HALF_TOP), reach_out.shape)
        else:
            scale[...] = HALF_TOP / (size * reach)

    force = own_rows[...].astype(jnp.float32) * pull[...]
    force = force + jnp.dot(w_s[...], s_slots[...], preferred_element_type=jnp.float32)
    force = force + jnp.dot(w_c[...], t_slots[...], preferred_element_type=jnp.float32)
    out[...] = force * scale[...]


def force_of(put, own_rows, weights, s_slots, t_slots, ways, spot=None):
    own = spot is not None
    rows = put.shape[0]
    slots, part = s_slots.shape
    size = min(part, 512)
    steps = part // size
    full = lambda shape: pl.BlockSpec(shape, lambda c, spot: (0, 0))
    cols = lambda high: pl.BlockSpec((high, size), lambda c, spot: (0, c))
    if own:
        out_specs = [
            pl.BlockSpec((rows, size), lambda c, spot: (0, spot[0] * steps + c)),
            full((rows, SLOTS)),
        ]
        out_shape = [
            jax.ShapeDtypeStruct((rows, part * ways), jnp.float32),
            jax.ShapeDtypeStruct((rows, SLOTS), jnp.float32),
        ]
    else:
        out_specs = cols(rows)
        out_shape = jax.ShapeDtypeStruct((rows, part), jnp.float32)
        spot = jnp.zeros((), jnp.int32)
    return pl.pallas_call(
        functools.partial(force_kernel, own),
        grid_spec=pltpu.PrefetchScalarGridSpec(
            num_scalar_prefetch=1,
            grid=(steps,),
            in_specs=[full((rows, slots)), cols(rows), full(weights.shape), cols(slots), cols(slots)],
            out_specs=out_specs,
            scratch_shapes=[
                pltpu.VMEM((rows, slots), jnp.bfloat16),
                pltpu.VMEM((rows, slots), jnp.bfloat16),
                pltpu.VMEM((rows, 1), jnp.float32),
                pltpu.VMEM((rows, 1), jnp.float32),
            ],
        ),
        out_shape=out_shape,
        cost_estimate=pl.CostEstimate(flops=4 * rows * slots * part, bytes_accessed=4 * slots * part, transcendentals=0),
        name="force_own" if own else "force",
    )(spot.reshape(1), put, own_rows, weights, s_slots, t_slots)


def grouped(student, teacher, bw_table, bw_index, group_ids, counts):
    ways = lax.axis_size("pair")
    pair = lax.axis_index("pair")
    rows, width = student.shape
    part = width // ways
    samples = rows * ways
    slots = GROUPS * SLOTS
    latent = float(width * lax.axis_size("value"))
    far_first = sorted(range(1, ways), key=lambda k: -k)
    chunks = CHUNKS if part % (CHUNKS * SLOTS) == 0 else 1
    size = part // chunks

    arrived = []
    for x in (student, teacher):
        for c in range(chunks):
            if len(arrived) >= 2:
                x, arrived[-2] = lax.optimization_barrier((x, arrived[-2]))
            arrived.append(exchange(x, pair, ways, c * size, size, far_first))
    student_k, teacher_k = arrived[:chunks], arrived[chunks:]

    same = group_ids[:, None] == group_ids[None, :]
    ids = jnp.arange(samples, dtype=jnp.int32)
    place = jnp.sum(same & (ids[None, :] < ids[:, None]), axis=1, dtype=jnp.int32)
    slot = group_ids * SLOTS + place
    slot_k = jnp.concatenate([lax.dynamic_slice_in_dim(slot, (pair ^ k) * rows, rows) for k in range(ways)])
    spots = jnp.arange(slots, dtype=jnp.int32)
    pick = (spots[:, None] == slot_k[None, :]).astype(jnp.bfloat16)
    put = (slot_k[:, None] == spots[None, :]).astype(jnp.bfloat16)

    def slotted(chunked):
        carry = None
        for c in range(chunks):
            carry = to_slots(pick, chunked[c], carry, c, chunks, part)
        return carry

    def gram(a, b):
        a, b = (x.reshape(GROUPS, SLOTS, part) for x in (a, b))
        return jnp.einsum("gsv,gtv->gst", a, b, preferred_element_type=jnp.float32)

    student_s = slotted(student_k)
    gram_self = all_sum(gram(student_s, student_s).reshape(slots, SLOTS)).reshape(GROUPS, SLOTS, SLOTS)
    teacher_s = slotted(teacher_k)
    eye = jnp.eye(SLOTS, dtype=jnp.float32)
    norm_t = jnp.sum(gram(teacher_s, teacher_s) * eye, axis=1, keepdims=True)
    cross = jnp.concatenate(
        [gram(student_s, teacher_s), jnp.broadcast_to(norm_t, (GROUPS, PAD, SLOTS))], axis=1
    )
    cross = all_sum(cross.reshape(-1, SLOTS)).reshape(GROUPS, SLOTS + PAD, SLOTS)

    weights, loss = weights_of(gram_self, cross, counts, bw_table, bw_index, latent)
    loss = jnp.sum(loss[0]) / samples

    def force_to(k, spot=None):
        rows_k = jnp.concatenate([student_k[c][k] for c in range(chunks)], axis=1)
        return force_of(put[k * rows : (k + 1) * rows], rows_k, weights, student_s, teacher_s, ways, spot)

    sent = {k: swap(force_to(k).astype(jnp.float16), "pair", k) for k in far_first}
    out, reach = force_to(0, pair)
    for k in far_first:
        block = sent[k].astype(jnp.float32) * reach[:, :1]
        out = lax.dynamic_update_slice_in_dim(out, block, (pair ^ k) * part, 1)
    return (out, loss)


def per_device(student, teacher, bw_table, bw_index, group_ids):
    counts = jnp.sum(
        group_ids[None, :] == jnp.arange(GROUPS, dtype=jnp.int32)[:, None], axis=1, dtype=jnp.int32
    )
    args = (student, teacher, bw_table, bw_index, group_ids)
    force, loss = grouped(*args, counts)
    state = (jnp.max(counts) > SLOTS, force, loss)
    state = lax.while_loop(lambda s: s[0], lambda s: (jnp.zeros((), bool), *general(*args)), state)
    return state[1:]


def solution(mesh):
    placed_in = (P("pair", "value"), P("pair", "value"), P(), P(), P())
    return jax.shard_map(
        per_device, mesh=mesh, in_specs=placed_in, out_specs=(P("pair", "value"), P()), check_vma=False
    )
```

```python
import functools

import jax
import jax.numpy as jnp
from jax import lax
from jax.experimental import pallas as pl
from jax.experimental.pallas import tpu as pltpu
from jax.sharding import PartitionSpec as P

GROUPS = 16
SLOTS = 128
ROWS = 512
PAD = 16
HALF_TOP = 32768.0
CHUNKS = 4


def kernel_terms(
    gram_self, gram_cross, norm_rows, norm_student, norm_teacher, same_group, heights, latent
):
    dist_self = jnp.maximum(norm_rows[..., :, None] + norm_student[..., None, :] - 2.0 * gram_self, 0.0)
    dist_cross = jnp.maximum(norm_rows[..., :, None] + norm_teacher[..., None, :] - 2.0 * gram_cross, 0.0)
    kern_self = jnp.zeros_like(dist_self)
    kern_cross = jnp.zeros_like(dist_cross)
    weight_self = jnp.zeros_like(dist_self)
    weight_cross = jnp.zeros_like(dist_cross)
    count = heights.shape[0]
    for member in range(count):
        height = heights[member]
        width_now = height * latent
        exp_self = jnp.exp(-dist_self / width_now)
        exp_cross = jnp.exp(-dist_cross / width_now)
        kern_self = kern_self + exp_self
        kern_cross = kern_cross + exp_cross
        weight_self = weight_self + exp_self / height
        weight_cross = weight_cross + exp_cross / height
    kern_self = kern_self / count * same_group
    kern_cross = kern_cross / count * same_group
    weight_self = weight_self / count * same_group
    weight_cross = weight_cross / count * same_group
    row_loss = jnp.sum(kern_self - 2.0 * kern_cross, axis=-1)
    total_self = jnp.sum(weight_self, axis=-1)
    total_cross = jnp.sum(weight_cross, axis=-1)
    return (
        weight_self.astype(jnp.bfloat16),
        weight_cross.astype(jnp.bfloat16),
        row_loss,
        total_self,
        total_cross,
    )


def pick_heights(bw_table, bw_index):
    table_slots = jnp.arange(bw_table.shape[0], dtype=jnp.int32)
    return jnp.sum(
        jnp.where(bw_index[:, None] == table_slots[None, :], bw_table[None, :], 0.0), axis=1
    )


def swap(x, axis, bits):
    count = lax.axis_size(axis)
    return lax.ppermute(x, axis, [(i, i ^ bits) for i in range(count)])


def take(x, index):
    return lax.dynamic_index_in_dim(x, index, 0, keepdims=False)


def placed(parts, me):
    x = jnp.stack(parts)
    bit = 1
    while bit < len(parts):
        order = [i ^ bit for i in range(len(parts))]
        x = jnp.where((me & bit) != 0, jnp.stack([x[i] for i in order]), x)
        bit *= 2
    return x


def reduce_stages():
    values = lax.axis_size("value")
    value = lax.axis_index("value")
    pair = lax.axis_index("pair")
    stages = [("value", 1, min(values, 2), value & 1)]
    stages.append(("pair", 1, lax.axis_size("pair"), pair))
    if values >= 8:
        stages.append(("value", 2, 4, (value >> 1) & 3))
        done = 8
    else:
        done = 2
    rest = []
    while done < values:
        rest.append(done)
        done *= 2
    return stages, rest


def all_sum(x):
    stages, rest = reduce_stages()
    for axis, unit, ways, me in stages:
        x = x.reshape((ways, x.shape[0] // ways) + x.shape[1:])
        got = [swap(take(x, me ^ k), axis, unit * k) for k in range(1, ways)]
        x = sum(got, take(x, me))
    for bits in rest:
        x = x + swap(x, "value", bits)
    for axis, unit, ways, me in reversed(stages):
        got = [x] + [swap(x, axis, unit * k) for k in range(1, ways)]
        x = placed(got, me)
        x = x.reshape((x.shape[0] * x.shape[1],) + x.shape[2:])
    return x


def pieces_of(x, pair, ways, lo, size):
    part = x.shape[1] // ways
    return [lax.dynamic_slice_in_dim(x, (pair ^ k) * part + lo, size, 1) for k in range(ways)]


def exchange(x, pair, ways, lo, size, order):
    pieces = pieces_of(x, pair, ways, lo, size)
    got = {0: pieces[0]}
    for k in order:
        got[k] = swap(pieces[k], "pair", k)
    return [got[k] for k in range(ways)]


def general(student, teacher, bw_table, bw_index, group_ids):
    ways = lax.axis_size("pair")
    pair = lax.axis_index("pair")
    rows, width = student.shape
    part = width // ways
    samples = rows * ways
    latent = float(width * lax.axis_size("value"))
    order = list(range(1, ways))
    block = SLOTS

    def gathered(x):
        full = jnp.zeros((samples, part), x.dtype)
        for k, got in enumerate(exchange(x, pair, ways, 0, part, order)):
            full = lax.dynamic_update_slice_in_dim(full, got, (pair ^ k) * rows, 0)
        return full

    def lane_sum(x):
        flat = x.reshape(-1, SLOTS)
        padded = jnp.pad(flat, ((0, -flat.shape[0] % 256), (0, 0)))
        return all_sum(padded)[: flat.shape[0]].reshape(x.shape)

    student_all, teacher_all = gathered(student), gathered(teacher)
    norms = jnp.stack([jnp.sum(x.astype(jnp.float32) ** 2, axis=1) for x in (student_all, teacher_all)])
    norm_student, norm_teacher = lane_sum(norms)
    heights = pick_heights(bw_table, bw_index)
    dims = (((1,), (1,)), ((), ()))

    def step(b, state):
        force, loss = state
        own = lax.dynamic_slice_in_dim(student_all, b * block, block)
        grams = [
            lax.dot_general(own, x, dims, preferred_element_type=jnp.float32) for x in (student_all, teacher_all)
        ]
        gram_self, gram_cross = lane_sum(jnp.stack(grams))
        own_ids = lax.dynamic_slice_in_dim(group_ids, b * block, block)
        same_group = (own_ids[:, None] == group_ids[None, :]).astype(jnp.float32)
        group_sizes = jnp.sum(same_group, axis=1)
        norm_rows = lax.dynamic_slice_in_dim(norm_student, b * block, block)
        weight_self, weight_cross, row_loss, total_self, total_cross = kernel_terms(
            gram_self, gram_cross, norm_rows, norm_student, norm_teacher, same_group, heights, latent
        )
        pulled = own.astype(jnp.float32) * (total_cross - total_self)[:, None]
        pulled = pulled + jnp.dot(weight_self, student_all, preferred_element_type=jnp.float32)
        pulled = pulled - jnp.dot(weight_cross, teacher_all, preferred_element_type=jnp.float32)
        pulled = pulled / group_sizes[:, None]
        force = lax.dynamic_update_slice_in_dim(force, pulled, b * block, 0)
        return force, loss + jnp.sum(row_loss / group_sizes)

    start = (jnp.zeros((samples, part), jnp.float32), jnp.zeros((), jnp.float32))
    force, loss = lax.fori_loop(0, samples // block, step, start)
    force = force.reshape(ways, rows, part)
    out = jnp.zeros((rows, width), jnp.float32)
    for k in range(ways):
        sent = take(force, pair ^ k)
        sent = swap(sent, "pair", k) if k else sent
        out = lax.dynamic_update_slice_in_dim(out, sent, (pair ^ k) * part, 1)
    return (out, loss / samples)


def slot_kernel(ways, first, *refs):
    pick, refs = refs[0], refs[1:]
    blocks, refs = refs[:ways], refs[ways:]
    slots_out, held = refs if first else refs[1:]
    rows = blocks[0].shape[0]

    @pl.when(pl.program_id(0) == 0)
    def _():
        for k in range(ways):
            held[k * rows : (k + 1) * rows] = blocks[k][...]

    slots_out[...] = jnp.dot(pick[...], held[...], preferred_element_type=jnp.float32).astype(jnp.bfloat16)


def to_slots(pick, blocks, carry, low, part):
    ways = len(blocks)
    rows, size = blocks[0].shape
    slots = pick.shape[0]
    first = carry is None
    chunk = low // size
    in_specs = [pl.BlockSpec((ROWS, ways * rows), lambda i: (i, 0))]
    in_specs += [pl.BlockSpec((rows, size), lambda i: (0, 0))] * ways
    args = [pick, *blocks]
    aliases = {}
    if not first:
        in_specs.append(pl.BlockSpec(memory_space=pl.ANY))
        aliases = {len(args): 0}
        args.append(carry)
    return pl.pallas_call(
        functools.partial(slot_kernel, ways, first),
        grid=(slots // ROWS,),
        in_specs=in_specs,
        out_specs=pl.BlockSpec((ROWS, size), lambda i: (i, chunk)),
        out_shape=jax.ShapeDtypeStruct((slots, part), jnp.bfloat16),
        scratch_shapes=[pltpu.VMEM((ways * rows, size), jnp.bfloat16)],
        input_output_aliases=aliases,
        cost_estimate=pl.CostEstimate(
            flops=2 * slots * size * ways * rows, bytes_accessed=slots * ways * rows * 2, transcendentals=0
        ),
        name="slots",
    )(*args)


def gram_kernel(cross, first, *refs):
    if cross:
        left, right = refs[:2]
        acc_in = None if first else refs[2]
        out = refs[-1]
    else:
        left = right = refs[0]
        acc_in, out = None, refs[-1]

    @pl.when(pl.program_id(1) == 0)
    def _():
        out[...] = jnp.zeros_like(out) if first else acc_in[...]

    dims = (((1,), (1,)), ((), ()))
    row = lax.broadcasted_iota(jnp.int32, (SLOTS, SLOTS), 0)
    col = lax.broadcasted_iota(jnp.int32, (SLOTS, SLOTS), 1)
    for g in range(out.shape[0]):
        at = slice(g * SLOTS, (g + 1) * SLOTS)
        own = right[at]
        if not cross:
            out[g] += lax.dot_general(own, own, dims, preferred_element_type=jnp.float32)
            continue
        both = jnp.concatenate([left[at], own], axis=0)
        gram = lax.dot_general(both, own, dims, preferred_element_type=jnp.float32)
        norm = jnp.sum(jnp.where(row == col, gram[SLOTS:], 0.0), axis=0, keepdims=True)
        out[g, :SLOTS] += gram[:SLOTS]
        out[g, SLOTS:] += jnp.broadcast_to(norm, (PAD, SLOTS))


def gram_of(left, right, carry, low, high, size):
    cross = right is not None
    first = carry is None
    tall = SLOTS + (PAD if cross else 0)
    held = ROWS // SLOTS
    cols = pl.BlockSpec((ROWS, size), lambda i, c: (i, low // size + c))
    block = pl.BlockSpec((held, tall, SLOTS), lambda i, c: (i, 0, 0))
    args = [left] + ([right] if cross else []) + ([] if first else [carry])
    slots = left.shape[0]
    return pl.pallas_call(
        functools.partial(gram_kernel, cross, first),
        grid=(slots // ROWS, (high - low) // size),
        in_specs=[cols] * (2 if cross else 1) + ([] if first else [block]),
        out_specs=block,
        out_shape=jax.ShapeDtypeStruct((GROUPS, tall, SLOTS), jnp.float32),
        cost_estimate=pl.CostEstimate(
            flops=8 * slots * SLOTS * (high - low), bytes_accessed=4 * slots * (high - low), transcendentals=0
        ),
        name="gram",
    )(*args)


def weight_kernel(latent, counts, index, table, self_ref, cross_ref, out, loss):
    step = pl.program_id(0)
    row = lax.broadcasted_iota(jnp.int32, (SLOTS, SLOTS), 0)
    col = lax.broadcasted_iota(jnp.int32, (SLOTS, SLOTS), 1)
    members = index.shape[0]
    scale = [-1.0 / (table[index[m]] * latent) for m in range(members)]
    inverse = [1.0 / (table[index[m]] * members) for m in range(members)]

    @pl.when(step == 0)
    def _():
        loss[...] = jnp.zeros_like(loss)

    for g in range(self_ref.shape[0]):
        size = counts[step * self_ref.shape[0] + g]
        used = (row < size) & (col < size)
        gram_self = self_ref[g]
        diag = jnp.where(row == col, gram_self, 0.0)
        norm_col = jnp.sum(diag, axis=0, keepdims=True)
        norm_row = jnp.sum(diag, axis=1, keepdims=True)

        def terms(gram, norm):
            both = norm_row + norm
            dist = jnp.maximum(both - 2.0 * gram, 0.0)
            kern = jnp.zeros_like(dist)
            weight = jnp.zeros_like(dist)
            for m in range(members):
                e = jnp.exp(dist * scale[m])
                kern = kern + e
                weight = weight + e * inverse[m]
            kern = jnp.where(used, kern, 0.0)
            weight = jnp.where(used, weight, 0.0)
            span = dist + both * (2.0 ** -10) + 1e-30
            return kern, weight, weight * (span * lax.rsqrt(span))

        kern_s, weight_s, reach_s = terms(gram_self, norm_col)
        kern_c, weight_c, reach_c = terms(cross_ref[g, :SLOTS], cross_ref[g, SLOTS : SLOTS + 1])
        count = jnp.maximum(size, 1).astype(jnp.float32)
        pull = jnp.sum(weight_c - weight_s, axis=1, keepdims=True)
        reach = jnp.sum(reach_s + reach_c, axis=1, keepdims=True) * (1.01 / count)
        reach = jnp.maximum(reach, 1e-30).astype(jnp.bfloat16).astype(jnp.float32)
        high = pull.astype(jnp.bfloat16).astype(jnp.float32)
        mid = (pull - high).astype(jnp.bfloat16).astype(jnp.float32)
        low = pull - high - mid
        extra = jnp.where(col == 0, high, jnp.where(col == 1, mid, jnp.where(col == 2, low, 0.0)))
        extra = jnp.where(col == 3, count, jnp.where(col == 4, reach, extra))
        at = slice(g * SLOTS, (g + 1) * SLOTS)
        out[at, :SLOTS] = weight_s.astype(jnp.bfloat16)
        out[at, SLOTS : 2 * SLOTS] = (-weight_c).astype(jnp.bfloat16)
        out[at, 2 * SLOTS :] = extra.astype(jnp.bfloat16)
        part = jnp.sum(kern_s - 2.0 * kern_c, axis=0, keepdims=True) * (1.0 / (count * members))
        loss[...] += jnp.broadcast_to(part, loss.shape)


def weights_of(gram_self, cross, counts, bw_table, bw_index, latent):
    smem = pl.BlockSpec(memory_space=pltpu.SMEM)
    high = cross.shape[1]
    held = 4
    return pl.pallas_call(
        functools.partial(weight_kernel, latent),
        grid=(GROUPS // held,),
        in_specs=[
            smem,
            smem,
            smem,
            pl.BlockSpec((held, SLOTS, SLOTS), lambda g: (g, 0, 0)),
            pl.BlockSpec((held, high, SLOTS), lambda g: (g, 0, 0)),
        ],
        out_specs=[
            pl.BlockSpec((held * SLOTS, 3 * SLOTS), lambda g: (g, 0)),
            pl.BlockSpec((8, SLOTS), lambda g: (0, 0)),
        ],
        out_shape=[
            jax.ShapeDtypeStruct((GROUPS * SLOTS, 3 * SLOTS), jnp.bfloat16),
            jax.ShapeDtypeStruct((8, SLOTS), jnp.float32),
        ],
        cost_estimate=pl.CostEstimate(flops=GROUPS * SLOTS * SLOTS * 60, bytes_accessed=4 << 20, transcendentals=0),
        name="weights",
    )(counts, bw_index, bw_table, gram_self, cross)


def force_kernel(own, spot, put, own_rows, weights, s_slots, t_slots, *refs):
    if own:
        out, reach_out, w_s, w_c, pull, scale = refs
    else:
        out, w_s, w_c, pull, scale = refs
    rows, slots = put.shape

    @pl.when(pl.program_id(0) == 0)
    def _():
        extra = jnp.zeros((rows, SLOTS), jnp.float32)
        for g in range(slots // SLOTS):
            at = slice(g * SLOTS, (g + 1) * SLOTS)
            found = jnp.dot(put[:, at], weights[at], preferred_element_type=jnp.float32)
            w_s[:, at] = found[:, :SLOTS].astype(jnp.bfloat16)
            w_c[:, at] = found[:, SLOTS : 2 * SLOTS].astype(jnp.bfloat16)
            extra = extra + found[:, 2 * SLOTS :]
        pull[...] = extra[:, 0:1] + extra[:, 1:2] + extra[:, 2:3]
        size = extra[:, 3:4]
        reach = extra[:, 4:5]
        if own:
            scale[...] = 1.0 / size
            reach_out[...] = jnp.broadcast_to(reach * (1.0 / HALF_TOP), reach_out.shape)
        else:
            scale[...] = HALF_TOP / (size * reach)

    force = own_rows[...].astype(jnp.float32) * pull[...]
    force = force + jnp.dot(w_s[...], s_slots[...], preferred_element_type=jnp.float32)
    force = force + jnp.dot(w_c[...], t_slots[...], preferred_element_type=jnp.float32)
    out[...] = force * scale[...]


def force_of(put, own_rows, weights, s_slots, t_slots, ways, spot=None):
    own = spot is not None
    rows = put.shape[0]
    slots, part = s_slots.shape
    size = min(part, 512)
    steps = part // size
    full = lambda shape: pl.BlockSpec(shape, lambda c, spot: (0, 0))
    cols = lambda high: pl.BlockSpec((high, size), lambda c, spot: (0, c))
    if own:
        out_specs = [
            pl.BlockSpec((rows, size), lambda c, spot: (0, spot[0] * steps + c)),
            full((rows, SLOTS)),
        ]
        out_shape = [
            jax.ShapeDtypeStruct((rows, part * ways), jnp.float32),
            jax.ShapeDtypeStruct((rows, SLOTS), jnp.float32),
        ]
    else:
        out_specs = cols(rows)
        out_shape = jax.ShapeDtypeStruct((rows, part), jnp.float32)
        spot = jnp.zeros((), jnp.int32)
    return pl.pallas_call(
        functools.partial(force_kernel, own),
        grid_spec=pltpu.PrefetchScalarGridSpec(
            num_scalar_prefetch=1,
            grid=(steps,),
            in_specs=[full((rows, slots)), cols(rows), full(weights.shape), cols(slots), cols(slots)],
            out_specs=out_specs,
            scratch_shapes=[
                pltpu.VMEM((rows, slots), jnp.bfloat16),
                pltpu.VMEM((rows, slots), jnp.bfloat16),
                pltpu.VMEM((rows, 1), jnp.float32),
                pltpu.VMEM((rows, 1), jnp.float32),
            ],
        ),
        out_shape=out_shape,
        cost_estimate=pl.CostEstimate(flops=4 * rows * slots * part, bytes_accessed=4 * slots * part, transcendentals=0),
        name="force_own" if own else "force",
    )(spot.reshape(1), put, own_rows, weights, s_slots, t_slots)


def grouped(student, teacher, bw_table, bw_index, group_ids, counts):
    ways = lax.axis_size("pair")
    pair = lax.axis_index("pair")
    rows, width = student.shape
    part = width // ways
    samples = rows * ways
    slots = GROUPS * SLOTS
    latent = float(width * lax.axis_size("value"))
    far_first = sorted(range(1, ways), key=lambda k: -k)
    size = part // CHUNKS if part % (CHUNKS * 2 * SLOTS) == 0 else part
    student_cuts = [(c * size, size) for c in range(part // size)]
    teacher_cuts = list(student_cuts)
    if size < part:
        teacher_cuts[-1:] = [(part - size, size // 2), (part - size // 2, size // 2)]

    arrived = []
    for x, cuts in ((student, student_cuts), (teacher, teacher_cuts)):
        for low, wide in cuts:
            if len(arrived) >= 2:
                x, arrived[-2] = lax.optimization_barrier((x, arrived[-2]))
            arrived.append(exchange(x, pair, ways, low, wide, far_first))
    chunks = len(student_cuts)
    student_k, teacher_k = arrived[:chunks], arrived[chunks:]

    same = group_ids[:, None] == group_ids[None, :]
    ids = jnp.arange(samples, dtype=jnp.int32)
    place = jnp.sum(same & (ids[None, :] < ids[:, None]), axis=1, dtype=jnp.int32)
    slot = group_ids * SLOTS + place
    slot_k = jnp.concatenate([lax.dynamic_slice_in_dim(slot, (pair ^ k) * rows, rows) for k in range(ways)])
    spots = jnp.arange(slots, dtype=jnp.int32)
    pick = (spots[:, None] == slot_k[None, :]).astype(jnp.bfloat16)
    put = (slot_k[:, None] == spots[None, :]).astype(jnp.bfloat16)

    def slotted(chunked, cuts, carry=None):
        for blocks, (low, _) in zip(chunked, cuts):
            carry = to_slots(pick, blocks, carry, low, part)
        return carry

    student_s = slotted(student_k, student_cuts)
    gram_self = gram_of(student_s, None, None, 0, part, size)
    gram_self = all_sum(gram_self.reshape(slots, SLOTS)).reshape(GROUPS, SLOTS, SLOTS)
    cross = None
    teacher_s = None
    low, wide = teacher_cuts[-1]
    if low:
        teacher_s = slotted(teacher_k[:-1], teacher_cuts[:-1])
        cross = gram_of(student_s, teacher_s, None, 0, low, wide)
        gram_self, cross, teacher_k[-1] = lax.optimization_barrier((gram_self, cross, teacher_k[-1]))
    teacher_s = slotted(teacher_k[-1:], teacher_cuts[-1:], teacher_s)
    cross = gram_of(student_s, teacher_s, cross, low, part, wide)
    cross = all_sum(cross.reshape(-1, SLOTS)).reshape(GROUPS, SLOTS + PAD, SLOTS)

    weights, loss = weights_of(gram_self, cross, counts, bw_table, bw_index, latent)
    loss = jnp.sum(loss[0]) / samples

    group_k = slot_k // SLOTS
    groups = jnp.arange(GROUPS, dtype=jnp.int32)

    def rows_of(k):
        return jnp.concatenate([student_k[c][k] for c in range(chunks)], axis=1)

    sent = {}
    for k in far_first:
        at = slice(k * rows, (k + 1) * rows)
        found = jnp.dot(put[at], weights, preferred_element_type=jnp.float32)
        here = group_k[at][:, None] == groups[None, :]
        w_s, w_c = (
            jnp.where(here[:, :, None], found[:, None, i * SLOTS : (i + 1) * SLOTS], 0.0)
            .astype(jnp.bfloat16)
            .reshape(rows, slots)
            for i in range(2)
        )
        extra = found[:, 2 * SLOTS :]
        pull = extra[:, 0:1] + extra[:, 1:2] + extra[:, 2:3]
        scale = HALF_TOP / (extra[:, 3:4] * extra[:, 4:5])
        f = rows_of(k).astype(jnp.float32) * pull
        f = f + jnp.dot(w_s, student_s, preferred_element_type=jnp.float32)
        f = f + jnp.dot(w_c, teacher_s, preferred_element_type=jnp.float32)
        sent[k] = swap((f * scale).astype(jnp.float16), "pair", k)
    out, reach = force_of(put[:rows], rows_of(0), weights, student_s, teacher_s, ways, pair)
    for k in far_first:
        block = sent[k].astype(jnp.float32) * reach[:, :1]
        out = lax.dynamic_update_slice_in_dim(out, block, (pair ^ k) * part, 1)
    return (out, loss)


def per_device(student, teacher, bw_table, bw_index, group_ids):
    counts = jnp.sum(
        group_ids[None, :] == jnp.arange(GROUPS, dtype=jnp.int32)[:, None], axis=1, dtype=jnp.int32
    )
    args = (student, teacher, bw_table, bw_index, group_ids)
    force, loss = grouped(*args, counts)
    state = (jnp.max(counts) > SLOTS, force, loss)
    state = lax.while_loop(lambda s: s[0], lambda s: (jnp.zeros((), bool), *general(*args)), state)
    return state[1:]


def solution(mesh):
    placed_in = (P("pair", "value"), P("pair", "value"), P(), P(), P())
    return jax.shard_map(
        per_device, mesh=mesh, in_specs=placed_in, out_specs=(P("pair", "value"), P()), check_vma=False
    )
```

```python
import functools

import jax
import jax.numpy as jnp
from jax import lax
from jax.experimental import pallas as pl
from jax.experimental.pallas import tpu as pltpu
from jax.sharding import PartitionSpec as P

GROUPS = 16
SLOTS = 128
ROWS = 512
PAD = 16
HALF_TOP = 32768.0
FLIGHT = 4
CHUNKS = 4


def kernel_terms(
    gram_self, gram_cross, norm_rows, norm_student, norm_teacher, same_group, heights, latent
):
    dist_self = jnp.maximum(norm_rows[..., :, None] + norm_student[..., None, :] - 2.0 * gram_self, 0.0)
    dist_cross = jnp.maximum(norm_rows[..., :, None] + norm_teacher[..., None, :] - 2.0 * gram_cross, 0.0)
    kern_self = jnp.zeros_like(dist_self)
    kern_cross = jnp.zeros_like(dist_cross)
    weight_self = jnp.zeros_like(dist_self)
    weight_cross = jnp.zeros_like(dist_cross)
    count = heights.shape[0]
    for member in range(count):
        height = heights[member]
        width_now = height * latent
        exp_self = jnp.exp(-dist_self / width_now)
        exp_cross = jnp.exp(-dist_cross / width_now)
        kern_self = kern_self + exp_self
        kern_cross = kern_cross + exp_cross
        weight_self = weight_self + exp_self / height
        weight_cross = weight_cross + exp_cross / height
    kern_self = kern_self / count * same_group
    kern_cross = kern_cross / count * same_group
    weight_self = weight_self / count * same_group
    weight_cross = weight_cross / count * same_group
    row_loss = jnp.sum(kern_self - 2.0 * kern_cross, axis=-1)
    total_self = jnp.sum(weight_self, axis=-1)
    total_cross = jnp.sum(weight_cross, axis=-1)
    return (
        weight_self.astype(jnp.bfloat16),
        weight_cross.astype(jnp.bfloat16),
        row_loss,
        total_self,
        total_cross,
    )


def pick_heights(bw_table, bw_index):
    table_slots = jnp.arange(bw_table.shape[0], dtype=jnp.int32)
    return jnp.sum(
        jnp.where(bw_index[:, None] == table_slots[None, :], bw_table[None, :], 0.0), axis=1
    )


def swap(x, axis, bits):
    count = lax.axis_size(axis)
    return lax.ppermute(x, axis, [(i, i ^ bits) for i in range(count)])


def take(x, index):
    return lax.dynamic_index_in_dim(x, index, 0, keepdims=False)


def placed(parts, me):
    x = jnp.stack(parts)
    bit = 1
    while bit < len(parts):
        order = [i ^ bit for i in range(len(parts))]
        x = jnp.where((me & bit) != 0, jnp.stack([x[i] for i in order]), x)
        bit *= 2
    return x


def reduce_stages():
    values = lax.axis_size("value")
    value = lax.axis_index("value")
    pair = lax.axis_index("pair")
    stages = [("value", 1, min(values, 2), value & 1)]
    stages.append(("pair", 1, lax.axis_size("pair"), pair))
    if values >= 8:
        stages.append(("value", 2, 4, (value >> 1) & 3))
        done = 8
    else:
        done = 2
    rest = []
    while done < values:
        rest.append(done)
        done *= 2
    return stages, rest


def all_sum(x):
    stages, rest = reduce_stages()
    for axis, unit, ways, me in stages:
        x = x.reshape((ways, x.shape[0] // ways) + x.shape[1:])
        got = [swap(take(x, me ^ k), axis, unit * k) for k in range(1, ways)]
        x = sum(got, take(x, me))
    for bits in rest:
        x = x + swap(x, "value", bits)
    for axis, unit, ways, me in reversed(stages):
        got = [x] + [swap(x, axis, unit * k) for k in range(1, ways)]
        x = placed(got, me)
        x = x.reshape((x.shape[0] * x.shape[1],) + x.shape[2:])
    return x


def pieces_of(x, pair, ways, lo, size):
    part = x.shape[1] // ways
    return [lax.dynamic_slice_in_dim(x, (pair ^ k) * part + lo, size, 1) for k in range(ways)]


def exchange(x, pair, ways, lo, size, order):
    pieces = pieces_of(x, pair, ways, lo, size)
    got = {0: pieces[0]}
    for k in order:
        got[k] = swap(pieces[k], "pair", k)
    return [got[k] for k in range(ways)]


def general(student, teacher, bw_table, bw_index, group_ids):
    ways = lax.axis_size("pair")
    pair = lax.axis_index("pair")
    rows, width = student.shape
    part = width // ways
    samples = rows * ways
    latent = float(width * lax.axis_size("value"))
    order = list(range(1, ways))
    block = SLOTS

    def gathered(x):
        full = jnp.zeros((samples, part), x.dtype)
        for k, got in enumerate(exchange(x, pair, ways, 0, part, order)):
            full = lax.dynamic_update_slice_in_dim(full, got, (pair ^ k) * rows, 0)
        return full

    def lane_sum(x):
        flat = x.reshape(-1, SLOTS)
        padded = jnp.pad(flat, ((0, -flat.shape[0] % 256), (0, 0)))
        return all_sum(padded)[: flat.shape[0]].reshape(x.shape)

    student_all, teacher_all = gathered(student), gathered(teacher)
    norms = jnp.stack([jnp.sum(x.astype(jnp.float32) ** 2, axis=1) for x in (student_all, teacher_all)])
    norm_student, norm_teacher = lane_sum(norms)
    heights = pick_heights(bw_table, bw_index)
    dims = (((1,), (1,)), ((), ()))

    def step(b, state):
        force, loss = state
        own = lax.dynamic_slice_in_dim(student_all, b * block, block)
        grams = [
            lax.dot_general(own, x, dims, preferred_element_type=jnp.float32) for x in (student_all, teacher_all)
        ]
        gram_self, gram_cross = lane_sum(jnp.stack(grams))
        own_ids = lax.dynamic_slice_in_dim(group_ids, b * block, block)
        same_group = (own_ids[:, None] == group_ids[None, :]).astype(jnp.float32)
        group_sizes = jnp.sum(same_group, axis=1)
        norm_rows = lax.dynamic_slice_in_dim(norm_student, b * block, block)
        weight_self, weight_cross, row_loss, total_self, total_cross = kernel_terms(
            gram_self, gram_cross, norm_rows, norm_student, norm_teacher, same_group, heights, latent
        )
        pulled = own.astype(jnp.float32) * (total_cross - total_self)[:, None]
        pulled = pulled + jnp.dot(weight_self, student_all, preferred_element_type=jnp.float32)
        pulled = pulled - jnp.dot(weight_cross, teacher_all, preferred_element_type=jnp.float32)
        pulled = pulled / group_sizes[:, None]
        force = lax.dynamic_update_slice_in_dim(force, pulled, b * block, 0)
        return force, loss + jnp.sum(row_loss / group_sizes)

    start = (jnp.zeros((samples, part), jnp.float32), jnp.zeros((), jnp.float32))
    force, loss = lax.fori_loop(0, samples // block, step, start)
    force = force.reshape(ways, rows, part)
    out = jnp.zeros((rows, width), jnp.float32)
    for k in range(ways):
        sent = take(force, pair ^ k)
        sent = swap(sent, "pair", k) if k else sent
        out = lax.dynamic_update_slice_in_dim(out, sent, (pair ^ k) * part, 1)
    return (out, loss / samples)


def slot_kernel(ways, first, *refs):
    pick, refs = refs[0], refs[1:]
    blocks, refs = refs[:ways], refs[ways:]
    slots_out, held = refs if first else refs[1:]
    rows = blocks[0].shape[0]

    @pl.when(pl.program_id(0) == 0)
    def _():
        for k in range(ways):
            held[k * rows : (k + 1) * rows] = blocks[k][...]

    slots_out[...] = jnp.dot(pick[...], held[...], preferred_element_type=jnp.float32).astype(jnp.bfloat16)


def to_slots(pick, blocks, carry, chunk, chunks, part):
    ways = len(blocks)
    rows, size = blocks[0].shape
    slots = pick.shape[0]
    first = carry is None
    in_specs = [pl.BlockSpec((ROWS, ways * rows), lambda i: (i, 0))]
    in_specs += [pl.BlockSpec((rows, size), lambda i: (0, 0))] * ways
    args = [pick, *blocks]
    aliases = {}
    if not first:
        in_specs.append(pl.BlockSpec(memory_space=pl.ANY))
        aliases = {len(args): 0}
        args.append(carry)
    return pl.pallas_call(
        functools.partial(slot_kernel, ways, first),
        grid=(slots // ROWS,),
        in_specs=in_specs,
        out_specs=pl.BlockSpec((ROWS, size), lambda i: (i, chunk)),
        out_shape=jax.ShapeDtypeStruct((slots, part), jnp.bfloat16),
        scratch_shapes=[pltpu.VMEM((ways * rows, size), jnp.bfloat16)],
        input_output_aliases=aliases,
        cost_estimate=pl.CostEstimate(
            flops=2 * slots * size * ways * rows, bytes_accessed=slots * ways * rows * 2, transcendentals=0
        ),
        name="slots",
    )(*args)


def weight_kernel(latent, counts, index, table, self_ref, cross_ref, out, loss):
    step = pl.program_id(0)
    row = lax.broadcasted_iota(jnp.int32, (SLOTS, SLOTS), 0)
    col = lax.broadcasted_iota(jnp.int32, (SLOTS, SLOTS), 1)
    members = index.shape[0]
    scale = [-1.0 / (table[index[m]] * latent) for m in range(members)]
    inverse = [1.0 / (table[index[m]] * members) for m in range(members)]

    @pl.when(step == 0)
    def _():
        loss[...] = jnp.zeros_like(loss)

    for g in range(self_ref.shape[0]):
        size = counts[step * self_ref.shape[0] + g]
        used = (row < size) & (col < size)
        gram_self = self_ref[g]
        diag = jnp.where(row == col, gram_self, 0.0)
        norm_col = jnp.sum(diag, axis=0, keepdims=True)
        norm_row = jnp.sum(diag, axis=1, keepdims=True)

        def terms(gram, norm):
            both = norm_row + norm
            dist = jnp.maximum(both - 2.0 * gram, 0.0)
            kern = jnp.zeros_like(dist)
            weight = jnp.zeros_like(dist)
            for m in range(members):
                e = jnp.exp(dist * scale[m])
                kern = kern + e
                weight = weight + e * inverse[m]
            kern = jnp.where(used, kern, 0.0)
            weight = jnp.where(used, weight, 0.0)
            span = dist + both * (2.0 ** -10) + 1e-30
            return kern, weight, weight * (span * lax.rsqrt(span))

        kern_s, weight_s, reach_s = terms(gram_self, norm_col)
        kern_c, weight_c, reach_c = terms(cross_ref[g, :SLOTS], cross_ref[g, SLOTS : SLOTS + 1])
        count = jnp.maximum(size, 1).astype(jnp.float32)
        pull = jnp.sum(weight_c - weight_s, axis=1, keepdims=True)
        reach = jnp.sum(reach_s + reach_c, axis=1, keepdims=True) * (1.01 / count)
        reach = jnp.maximum(reach, 1e-30).astype(jnp.bfloat16).astype(jnp.float32)
        high = pull.astype(jnp.bfloat16).astype(jnp.float32)
        mid = (pull - high).astype(jnp.bfloat16).astype(jnp.float32)
        low = pull - high - mid
        extra = jnp.where(col == 0, high, jnp.where(col == 1, mid, jnp.where(col == 2, low, 0.0)))
        extra = jnp.where(col == 3, count, jnp.where(col == 4, reach, extra))
        at = slice(g * SLOTS, (g + 1) * SLOTS)
        out[at, :SLOTS] = weight_s.astype(jnp.bfloat16)
        out[at, SLOTS : 2 * SLOTS] = (-weight_c).astype(jnp.bfloat16)
        out[at, 2 * SLOTS :] = extra.astype(jnp.bfloat16)
        part = jnp.sum(kern_s - 2.0 * kern_c, axis=0, keepdims=True) * (1.0 / (count * members))
        loss[...] += jnp.broadcast_to(part, loss.shape)


def weights_of(gram_self, cross, counts, bw_table, bw_index, latent):
    smem = pl.BlockSpec(memory_space=pltpu.SMEM)
    high = cross.shape[1]
    held = 4
    return pl.pallas_call(
        functools.partial(weight_kernel, latent),
        grid=(GROUPS // held,),
        in_specs=[
            smem,
            smem,
            smem,
            pl.BlockSpec((held, SLOTS, SLOTS), lambda g: (g, 0, 0)),
            pl.BlockSpec((held, high, SLOTS), lambda g: (g, 0, 0)),
        ],
        out_specs=[
            pl.BlockSpec((held * SLOTS, 3 * SLOTS), lambda g: (g, 0)),
            pl.BlockSpec((8, SLOTS), lambda g: (0, 0)),
        ],
        out_shape=[
            jax.ShapeDtypeStruct((GROUPS * SLOTS, 3 * SLOTS), jnp.bfloat16),
            jax.ShapeDtypeStruct((8, SLOTS), jnp.float32),
        ],
        cost_estimate=pl.CostEstimate(flops=GROUPS * SLOTS * SLOTS * 60, bytes_accessed=4 << 20, transcendentals=0),
        name="weights",
    )(counts, bw_index, bw_table, gram_self, cross)


def force_kernel(own, spot, put, own_rows, weights, s_slots, t_slots, *refs):
    if own:
        out, reach_out, w_s, w_c, pull, scale = refs
    else:
        out, w_s, w_c, pull, scale = refs
    rows, slots = put.shape

    @pl.when(pl.program_id(0) == 0)
    def _():
        extra = jnp.zeros((rows, SLOTS), jnp.float32)
        for g in range(slots // SLOTS):
            at = slice(g * SLOTS, (g + 1) * SLOTS)
            found = jnp.dot(put[:, at], weights[at], preferred_element_type=jnp.float32)
            w_s[:, at] = found[:, :SLOTS].astype(jnp.bfloat16)
            w_c[:, at] = found[:, SLOTS : 2 * SLOTS].astype(jnp.bfloat16)
            extra = extra + found[:, 2 * SLOTS :]
        pull[...] = extra[:, 0:1] + extra[:, 1:2] + extra[:, 2:3]
        size = extra[:, 3:4]
        reach = extra[:, 4:5]
        if own:
            scale[...] = 1.0 / size
            reach_out[...] = jnp.broadcast_to(reach * (1.0 / HALF_TOP), reach_out.shape)
        else:
            scale[...] = HALF_TOP / (size * reach)

    force = own_rows[...].astype(jnp.float32) * pull[...]
    force = force + jnp.dot(w_s[...], s_slots[...], preferred_element_type=jnp.float32)
    force = force + jnp.dot(w_c[...], t_slots[...], preferred_element_type=jnp.float32)
    out[...] = force * scale[...]


def force_of(put, own_rows, weights, s_slots, t_slots, ways, spot=None):
    own = spot is not None
    rows = put.shape[0]
    slots, part = s_slots.shape
    size = min(part, 512)
    steps = part // size
    full = lambda shape: pl.BlockSpec(shape, lambda c, spot: (0, 0))
    cols = lambda high: pl.BlockSpec((high, size), lambda c, spot: (0, c))
    if own:
        out_specs = [
            pl.BlockSpec((rows, size), lambda c, spot: (0, spot[0] * steps + c)),
            full((rows, SLOTS)),
        ]
        out_shape = [
            jax.ShapeDtypeStruct((rows, part * ways), jnp.float32),
            jax.ShapeDtypeStruct((rows, SLOTS), jnp.float32),
        ]
    else:
        out_specs = cols(rows)
        out_shape = jax.ShapeDtypeStruct((rows, part), jnp.float32)
        spot = jnp.zeros((), jnp.int32)
    return pl.pallas_call(
        functools.partial(force_kernel, own),
        grid_spec=pltpu.PrefetchScalarGridSpec(
            num_scalar_prefetch=1,
            grid=(steps,),
            in_specs=[full((rows, slots)), cols(rows), full(weights.shape), cols(slots), cols(slots)],
            out_specs=out_specs,
            scratch_shapes=[
                pltpu.VMEM((rows, slots), jnp.bfloat16),
                pltpu.VMEM((rows, slots), jnp.bfloat16),
                pltpu.VMEM((rows, 1), jnp.float32),
                pltpu.VMEM((rows, 1), jnp.float32),
            ],
        ),
        out_shape=out_shape,
        cost_estimate=pl.CostEstimate(flops=4 * rows * slots * part, bytes_accessed=4 * slots * part, transcendentals=0),
        name="force_own" if own else "force",
    )(spot.reshape(1), put, own_rows, weights, s_slots, t_slots)


def expand_kernel(put, weights, w_s, w_c, extra):
    found = jnp.dot(put[...], weights[...], preferred_element_type=jnp.float32)
    w_s[...] = found[:, :SLOTS].astype(jnp.bfloat16)
    w_c[...] = found[:, SLOTS : 2 * SLOTS].astype(jnp.bfloat16)

    @pl.when(pl.program_id(0) == 0)
    def _():
        extra[...] = jnp.zeros_like(extra)

    extra[...] += found[:, 2 * SLOTS :]


def expand(put, weights):
    high, slots = put.shape
    cols = pl.BlockSpec((high, SLOTS), lambda g: (0, g))
    return pl.pallas_call(
        expand_kernel,
        grid=(slots // SLOTS,),
        in_specs=[cols, pl.BlockSpec((SLOTS, 3 * SLOTS), lambda g: (g, 0))],
        out_specs=[cols, cols, pl.BlockSpec((high, SLOTS), lambda g: (0, 0))],
        out_shape=[
            jax.ShapeDtypeStruct((high, slots), jnp.bfloat16),
            jax.ShapeDtypeStruct((high, slots), jnp.bfloat16),
            jax.ShapeDtypeStruct((high, SLOTS), jnp.float32),
        ],
        cost_estimate=pl.CostEstimate(flops=6 * high * slots * SLOTS, bytes_accessed=6 * high * slots, transcendentals=0),
        name="expand",
    )(put, weights)


def columns_kernel(dests, w_s, w_c, extra, *refs):
    own_rows, (s_slots, t_slots, out) = refs[:dests], refs[dests:]
    parts = extra[...]
    pull = parts[:, 0:1] + parts[:, 1:2] + parts[:, 2:3]
    scale = HALF_TOP / (parts[:, 3:4] * parts[:, 4:5])
    products = jnp.dot(w_s[...], s_slots[...], preferred_element_type=jnp.float32)
    products = products + jnp.dot(w_c[...], t_slots[...], preferred_element_type=jnp.float32)
    for d in range(dests):

        @pl.when(pl.program_id(0) == d)
        def _():
            out[...] = (products + own_rows[d][...].astype(jnp.float32) * pull) * scale


def force_columns(chunk, w_s, w_c, extra, own_rows, s_slots, t_slots):
    dests = len(own_rows)
    rows, size = own_rows[0].shape
    slots = w_s.shape[1]
    cols = pl.BlockSpec((slots, size), lambda d: (0, chunk))
    row = lambda wide: pl.BlockSpec((rows, wide), lambda d: (d, 0))
    return pl.pallas_call(
        functools.partial(columns_kernel, dests),
        grid=(dests,),
        in_specs=[row(slots), row(slots), row(SLOTS)]
        + [pl.BlockSpec((rows, size), lambda d: (0, 0))] * dests
        + [cols, cols],
        out_specs=row(size),
        out_shape=jax.ShapeDtypeStruct((dests * rows, size), jnp.float32),
        cost_estimate=pl.CostEstimate(
            flops=4 * dests * rows * slots * size, bytes_accessed=4 * slots * size, transcendentals=0
        ),
        name="force_columns",
    )(w_s, w_c, extra, *own_rows, s_slots, t_slots)


def grouped(student, teacher, bw_table, bw_index, group_ids, counts):
    ways = lax.axis_size("pair")
    pair = lax.axis_index("pair")
    rows, width = student.shape
    part = width // ways
    samples = rows * ways
    slots = GROUPS * SLOTS
    latent = float(width * lax.axis_size("value"))
    far_first = sorted(range(1, ways), key=lambda k: -k)
    chunks = CHUNKS if part % (CHUNKS * SLOTS) == 0 else 1
    size = part // chunks

    arrived = []
    for x in (student, teacher):
        for c in range(chunks):
            if len(arrived) >= FLIGHT:
                x, arrived[-FLIGHT] = lax.optimization_barrier((x, arrived[-FLIGHT]))
            arrived.append(exchange(x, pair, ways, c * size, size, far_first))
    student_k, teacher_k = arrived[:chunks], arrived[chunks:]

    same = group_ids[:, None] == group_ids[None, :]
    ids = jnp.arange(samples, dtype=jnp.int32)
    place = jnp.sum(same & (ids[None, :] < ids[:, None]), axis=1, dtype=jnp.int32)
    slot = group_ids * SLOTS + place
    slot_k = jnp.concatenate([lax.dynamic_slice_in_dim(slot, (pair ^ k) * rows, rows) for k in range(ways)])
    spots = jnp.arange(slots, dtype=jnp.int32)
    pick = (spots[:, None] == slot_k[None, :]).astype(jnp.bfloat16)
    put = (slot_k[:, None] == spots[None, :]).astype(jnp.bfloat16)

    def slotted(chunked):
        carry = None
        for c in range(chunks):
            carry = to_slots(pick, chunked[c], carry, c, chunks, part)
        return carry

    def gram(a, b):
        a, b = (x.reshape(GROUPS, SLOTS, part) for x in (a, b))
        return jnp.einsum("gsv,gtv->gst", a, b, preferred_element_type=jnp.float32)

    student_s = slotted(student_k)
    gram_self = all_sum(gram(student_s, student_s).reshape(slots, SLOTS)).reshape(GROUPS, SLOTS, SLOTS)
    teacher_s = slotted(teacher_k)
    t_wide = teacher.astype(jnp.float32)
    norm_own = jnp.sum(t_wide * t_wide, axis=1)
    norm_t = jnp.sum(jnp.where(spots[:, None] == slot_k[None, :rows], norm_own[None, :], 0.0), axis=1)
    norm_t = norm_t.reshape(GROUPS, 1, SLOTS)
    cross = jnp.concatenate(
        [gram(student_s, teacher_s), jnp.broadcast_to(norm_t, (GROUPS, PAD, SLOTS))], axis=1
    )
    cross = all_sum(cross.reshape(-1, SLOTS)).reshape(GROUPS, SLOTS + PAD, SLOTS)

    weights, loss = weights_of(gram_self, cross, counts, bw_table, bw_index, latent)
    loss = jnp.sum(loss[0]) / samples

    def force_to(k, spot=None):
        rows_k = jnp.concatenate([student_k[c][k] for c in range(chunks)], axis=1)
        return force_of(put[k * rows : (k + 1) * rows], rows_k, weights, student_s, teacher_s, ways, spot)

    w_s, w_c, extra = expand(put[rows:], weights)
    ready = [
        force_columns(c, w_s, w_c, extra, [student_k[c][k] for k in range(1, ways)], student_s, teacher_s)
        for c in range(chunks)
    ]
    sent = [
        {k: swap(ready[c][(k - 1) * rows : k * rows].astype(jnp.float16), "pair", k) for k in far_first}
        for c in range(chunks)
    ]
    out, reach = force_to(0, pair)
    for c in range(chunks):
        for k in far_first:
            block = sent[c][k].astype(jnp.float32) * reach[:, :1]
            out = lax.dynamic_update_slice_in_dim(out, block, (pair ^ k) * part + c * size, 1)
    return (out, loss)


def per_device(student, teacher, bw_table, bw_index, group_ids):
    counts = jnp.sum(
        group_ids[None, :] == jnp.arange(GROUPS, dtype=jnp.int32)[:, None], axis=1, dtype=jnp.int32
    )
    args = (student, teacher, bw_table, bw_index, group_ids)
    force, loss = grouped(*args, counts)
    state = (jnp.max(counts) > SLOTS, force, loss)
    state = lax.while_loop(lambda s: s[0], lambda s: (jnp.zeros((), bool), *general(*args)), state)
    return state[1:]


def solution(mesh):
    placed_in = (P("pair", "value"), P("pair", "value"), P(), P(), P())
    return jax.shard_map(
        per_device, mesh=mesh, in_specs=placed_in, out_specs=(P("pair", "value"), P()), check_vma=False
    )
```

```python
import functools

import jax
import jax.numpy as jnp
from jax import lax
from jax.experimental import pallas as pl
from jax.experimental.pallas import tpu as pltpu
from jax.sharding import PartitionSpec as P

GROUPS = 16
SLOTS = 128
ROWS = 512
PAD = 16
HALF_TOP = 32768.0
FLIGHT = 4
CHUNKS = 4


def kernel_terms(
    gram_self, gram_cross, norm_rows, norm_student, norm_teacher, same_group, heights, latent
):
    dist_self = jnp.maximum(norm_rows[..., :, None] + norm_student[..., None, :] - 2.0 * gram_self, 0.0)
    dist_cross = jnp.maximum(norm_rows[..., :, None] + norm_teacher[..., None, :] - 2.0 * gram_cross, 0.0)
    kern_self = jnp.zeros_like(dist_self)
    kern_cross = jnp.zeros_like(dist_cross)
    weight_self = jnp.zeros_like(dist_self)
    weight_cross = jnp.zeros_like(dist_cross)
    count = heights.shape[0]
    for member in range(count):
        height = heights[member]
        width_now = height * latent
        exp_self = jnp.exp(-dist_self / width_now)
        exp_cross = jnp.exp(-dist_cross / width_now)
        kern_self = kern_self + exp_self
        kern_cross = kern_cross + exp_cross
        weight_self = weight_self + exp_self / height
        weight_cross = weight_cross + exp_cross / height
    kern_self = kern_self / count * same_group
    kern_cross = kern_cross / count * same_group
    weight_self = weight_self / count * same_group
    weight_cross = weight_cross / count * same_group
    row_loss = jnp.sum(kern_self - 2.0 * kern_cross, axis=-1)
    total_self = jnp.sum(weight_self, axis=-1)
    total_cross = jnp.sum(weight_cross, axis=-1)
    return (
        weight_self.astype(jnp.bfloat16),
        weight_cross.astype(jnp.bfloat16),
        row_loss,
        total_self,
        total_cross,
    )


def pick_heights(bw_table, bw_index):
    table_slots = jnp.arange(bw_table.shape[0], dtype=jnp.int32)
    return jnp.sum(
        jnp.where(bw_index[:, None] == table_slots[None, :], bw_table[None, :], 0.0), axis=1
    )


def swap(x, axis, bits):
    count = lax.axis_size(axis)
    return lax.ppermute(x, axis, [(i, i ^ bits) for i in range(count)])


def take(x, index):
    return lax.dynamic_index_in_dim(x, index, 0, keepdims=False)


def placed(parts, me):
    x = jnp.stack(parts)
    bit = 1
    while bit < len(parts):
        order = [i ^ bit for i in range(len(parts))]
        x = jnp.where((me & bit) != 0, jnp.stack([x[i] for i in order]), x)
        bit *= 2
    return x


def reduce_stages():
    values = lax.axis_size("value")
    value = lax.axis_index("value")
    pair = lax.axis_index("pair")
    stages = [("value", 1, min(values, 2), value & 1)]
    stages.append(("pair", 1, lax.axis_size("pair"), pair))
    if values >= 8:
        stages.append(("value", 2, 4, (value >> 1) & 3))
        done = 8
    else:
        done = 2
    rest = []
    while done < values:
        rest.append(done)
        done *= 2
    return stages, rest


def all_sum(x):
    stages, rest = reduce_stages()
    for axis, unit, ways, me in stages:
        x = x.reshape((ways, x.shape[0] // ways) + x.shape[1:])
        got = [swap(take(x, me ^ k), axis, unit * k) for k in range(1, ways)]
        x = sum(got, take(x, me))
    for bits in rest:
        x = x + swap(x, "value", bits)
    for axis, unit, ways, me in reversed(stages):
        got = [x] + [swap(x, axis, unit * k) for k in range(1, ways)]
        x = placed(got, me)
        x = x.reshape((x.shape[0] * x.shape[1],) + x.shape[2:])
    return x


def pieces_of(x, pair, ways, lo, size):
    part = x.shape[1] // ways
    return [lax.dynamic_slice_in_dim(x, (pair ^ k) * part + lo, size, 1) for k in range(ways)]


def exchange(x, pair, ways, lo, size, order):
    pieces = pieces_of(x, pair, ways, lo, size)
    got = {0: pieces[0]}
    for k in order:
        got[k] = swap(pieces[k], "pair", k)
    return [got[k] for k in range(ways)]


def general(student, teacher, bw_table, bw_index, group_ids):
    ways = lax.axis_size("pair")
    pair = lax.axis_index("pair")
    rows, width = student.shape
    part = width // ways
    samples = rows * ways
    latent = float(width * lax.axis_size("value"))
    order = list(range(1, ways))
    block = SLOTS

    def gathered(x):
        full = jnp.zeros((samples, part), x.dtype)
        for k, got in enumerate(exchange(x, pair, ways, 0, part, order)):
            full = lax.dynamic_update_slice_in_dim(full, got, (pair ^ k) * rows, 0)
        return full

    def lane_sum(x):
        flat = x.reshape(-1, SLOTS)
        padded = jnp.pad(flat, ((0, -flat.shape[0] % 256), (0, 0)))
        return all_sum(padded)[: flat.shape[0]].reshape(x.shape)

    student_all, teacher_all = gathered(student), gathered(teacher)
    norms = jnp.stack([jnp.sum(x.astype(jnp.float32) ** 2, axis=1) for x in (student_all, teacher_all)])
    norm_student, norm_teacher = lane_sum(norms)
    heights = pick_heights(bw_table, bw_index)
    dims = (((1,), (1,)), ((), ()))

    def step(b, state):
        force, loss = state
        own = lax.dynamic_slice_in_dim(student_all, b * block, block)
        grams = [
            lax.dot_general(own, x, dims, preferred_element_type=jnp.float32) for x in (student_all, teacher_all)
        ]
        gram_self, gram_cross = lane_sum(jnp.stack(grams))
        own_ids = lax.dynamic_slice_in_dim(group_ids, b * block, block)
        same_group = (own_ids[:, None] == group_ids[None, :]).astype(jnp.float32)
        group_sizes = jnp.sum(same_group, axis=1)
        norm_rows = lax.dynamic_slice_in_dim(norm_student, b * block, block)
        weight_self, weight_cross, row_loss, total_self, total_cross = kernel_terms(
            gram_self, gram_cross, norm_rows, norm_student, norm_teacher, same_group, heights, latent
        )
        pulled = own.astype(jnp.float32) * (total_cross - total_self)[:, None]
        pulled = pulled + jnp.dot(weight_self, student_all, preferred_element_type=jnp.float32)
        pulled = pulled - jnp.dot(weight_cross, teacher_all, preferred_element_type=jnp.float32)
        pulled = pulled / group_sizes[:, None]
        force = lax.dynamic_update_slice_in_dim(force, pulled, b * block, 0)
        return force, loss + jnp.sum(row_loss / group_sizes)

    start = (jnp.zeros((samples, part), jnp.float32), jnp.zeros((), jnp.float32))
    force, loss = lax.fori_loop(0, samples // block, step, start)
    force = force.reshape(ways, rows, part)
    out = jnp.zeros((rows, width), jnp.float32)
    for k in range(ways):
        sent = take(force, pair ^ k)
        sent = swap(sent, "pair", k) if k else sent
        out = lax.dynamic_update_slice_in_dim(out, sent, (pair ^ k) * part, 1)
    return (out, loss / samples)


def slot_kernel(ways, first, *refs):
    pick, refs = refs[0], refs[1:]
    blocks, refs = refs[:ways], refs[ways:]
    slots_out, held = refs if first else refs[1:]
    rows = blocks[0].shape[0]

    @pl.when(pl.program_id(0) == 0)
    def _():
        for k in range(ways):
            held[k * rows : (k + 1) * rows] = blocks[k][...]

    slots_out[...] = jnp.dot(pick[...], held[...], preferred_element_type=jnp.float32).astype(jnp.bfloat16)


def to_slots(pick, blocks, carry, chunk, chunks, part):
    ways = len(blocks)
    rows, size = blocks[0].shape
    slots = pick.shape[0]
    first = carry is None
    in_specs = [pl.BlockSpec((ROWS, ways * rows), lambda i: (i, 0))]
    in_specs += [pl.BlockSpec((rows, size), lambda i: (0, 0))] * ways
    args = [pick, *blocks]
    aliases = {}
    if not first:
        in_specs.append(pl.BlockSpec(memory_space=pl.ANY))
        aliases = {len(args): 0}
        args.append(carry)
    return pl.pallas_call(
        functools.partial(slot_kernel, ways, first),
        grid=(slots // ROWS,),
        in_specs=in_specs,
        out_specs=pl.BlockSpec((ROWS, size), lambda i: (i, chunk)),
        out_shape=jax.ShapeDtypeStruct((slots, part), jnp.bfloat16),
        scratch_shapes=[pltpu.VMEM((ways * rows, size), jnp.bfloat16)],
        input_output_aliases=aliases,
        cost_estimate=pl.CostEstimate(
            flops=2 * slots * size * ways * rows, bytes_accessed=slots * ways * rows * 2, transcendentals=0
        ),
        name="slots",
    )(*args)


def weight_kernel(latent, counts, index, table, self_ref, cross_ref, out, loss):
    step = pl.program_id(0)
    row = lax.broadcasted_iota(jnp.int32, (SLOTS, SLOTS), 0)
    col = lax.broadcasted_iota(jnp.int32, (SLOTS, SLOTS), 1)
    members = index.shape[0]
    scale = [-1.0 / (table[index[m]] * latent) for m in range(members)]
    inverse = [1.0 / (table[index[m]] * members) for m in range(members)]

    @pl.when(step == 0)
    def _():
        loss[...] = jnp.zeros_like(loss)

    for g in range(self_ref.shape[0]):
        size = counts[step * self_ref.shape[0] + g]
        used = (row < size) & (col < size)
        gram_self = self_ref[g]
        diag = jnp.where(row == col, gram_self, 0.0)
        norm_col = jnp.sum(diag, axis=0, keepdims=True)
        norm_row = jnp.sum(diag, axis=1, keepdims=True)

        def terms(gram, norm):
            both = norm_row + norm
            dist = jnp.maximum(both - 2.0 * gram, 0.0)
            kern = jnp.zeros_like(dist)
            weight = jnp.zeros_like(dist)
            for m in range(members):
                e = jnp.exp(dist * scale[m])
                kern = kern + e
                weight = weight + e * inverse[m]
            kern = jnp.where(used, kern, 0.0)
            weight = jnp.where(used, weight, 0.0)
            span = dist + both * (2.0 ** -10) + 1e-30
            return kern, weight, weight * (span * lax.rsqrt(span))

        kern_s, weight_s, reach_s = terms(gram_self, norm_col)
        kern_c, weight_c, reach_c = terms(cross_ref[g, :SLOTS], cross_ref[g, SLOTS : SLOTS + 1])
        count = jnp.maximum(size, 1).astype(jnp.float32)
        pull = jnp.sum(weight_c - weight_s, axis=1, keepdims=True)
        reach = jnp.sum(reach_s + reach_c, axis=1, keepdims=True) * (1.01 / count)
        reach = jnp.maximum(reach, 1e-30).astype(jnp.bfloat16).astype(jnp.float32)
        high = pull.astype(jnp.bfloat16).astype(jnp.float32)
        mid = (pull - high).astype(jnp.bfloat16).astype(jnp.float32)
        low = pull - high - mid
        extra = jnp.where(col == 0, high, jnp.where(col == 1, mid, jnp.where(col == 2, low, 0.0)))
        extra = jnp.where(col == 3, count, jnp.where(col == 4, reach, extra))
        at = slice(g * SLOTS, (g + 1) * SLOTS)
        out[at, :SLOTS] = weight_s.astype(jnp.bfloat16)
        out[at, SLOTS : 2 * SLOTS] = (-weight_c).astype(jnp.bfloat16)
        out[at, 2 * SLOTS :] = extra.astype(jnp.bfloat16)
        part = jnp.sum(kern_s - 2.0 * kern_c, axis=0, keepdims=True) * (1.0 / (count * members))
        loss[...] += jnp.broadcast_to(part, loss.shape)


def weights_of(gram_self, cross, counts, bw_table, bw_index, latent):
    smem = pl.BlockSpec(memory_space=pltpu.SMEM)
    high = cross.shape[1]
    held = 4
    return pl.pallas_call(
        functools.partial(weight_kernel, latent),
        grid=(GROUPS // held,),
        in_specs=[
            smem,
            smem,
            smem,
            pl.BlockSpec((held, SLOTS, SLOTS), lambda g: (g, 0, 0)),
            pl.BlockSpec((held, high, SLOTS), lambda g: (g, 0, 0)),
        ],
        out_specs=[
            pl.BlockSpec((held * SLOTS, 3 * SLOTS), lambda g: (g, 0)),
            pl.BlockSpec((8, SLOTS), lambda g: (0, 0)),
        ],
        out_shape=[
            jax.ShapeDtypeStruct((GROUPS * SLOTS, 3 * SLOTS), jnp.bfloat16),
            jax.ShapeDtypeStruct((8, SLOTS), jnp.float32),
        ],
        cost_estimate=pl.CostEstimate(flops=GROUPS * SLOTS * SLOTS * 60, bytes_accessed=4 << 20, transcendentals=0),
        name="weights",
    )(counts, bw_index, bw_table, gram_self, cross)


def force_kernel(own, spot, put, own_rows, weights, s_slots, t_slots, *refs):
    if own:
        out, reach_out, w_s, w_c, pull, scale = refs
    else:
        out, w_s, w_c, pull, scale = refs
    rows, slots = put.shape

    @pl.when(pl.program_id(0) == 0)
    def _():
        extra = jnp.zeros((rows, SLOTS), jnp.float32)
        for g in range(slots // SLOTS):
            at = slice(g * SLOTS, (g + 1) * SLOTS)
            found = jnp.dot(put[:, at], weights[at], preferred_element_type=jnp.float32)
            w_s[:, at] = found[:, :SLOTS].astype(jnp.bfloat16)
            w_c[:, at] = found[:, SLOTS : 2 * SLOTS].astype(jnp.bfloat16)
            extra = extra + found[:, 2 * SLOTS :]
        pull[...] = extra[:, 0:1] + extra[:, 1:2] + extra[:, 2:3]
        size = extra[:, 3:4]
        reach = extra[:, 4:5]
        if own:
            scale[...] = 1.0 / size
            reach_out[...] = jnp.broadcast_to(reach * (1.0 / HALF_TOP), reach_out.shape)
        else:
            scale[...] = HALF_TOP / (size * reach)

    force = own_rows[...].astype(jnp.float32) * pull[...]
    force = force + jnp.dot(w_s[...], s_slots[...], preferred_element_type=jnp.float32)
    force = force + jnp.dot(w_c[...], t_slots[...], preferred_element_type=jnp.float32)
    out[...] = force * scale[...]


def force_of(put, own_rows, weights, s_slots, t_slots, ways, spot=None):
    own = spot is not None
    rows = put.shape[0]
    slots, part = s_slots.shape
    size = min(part, 512)
    steps = part // size
    full = lambda shape: pl.BlockSpec(shape, lambda c, spot: (0, 0))
    cols = lambda high: pl.BlockSpec((high, size), lambda c, spot: (0, c))
    if own:
        out_specs = [
            pl.BlockSpec((rows, size), lambda c, spot: (0, spot[0] * steps + c)),
            full((rows, SLOTS)),
        ]
        out_shape = [
            jax.ShapeDtypeStruct((rows, part * ways), jnp.float32),
            jax.ShapeDtypeStruct((rows, SLOTS), jnp.float32),
        ]
    else:
        out_specs = cols(rows)
        out_shape = jax.ShapeDtypeStruct((rows, part), jnp.float32)
        spot = jnp.zeros((), jnp.int32)
    return pl.pallas_call(
        functools.partial(force_kernel, own),
        grid_spec=pltpu.PrefetchScalarGridSpec(
            num_scalar_prefetch=1,
            grid=(steps,),
            in_specs=[full((rows, slots)), cols(rows), full(weights.shape), cols(slots), cols(slots)],
            out_specs=out_specs,
            scratch_shapes=[
                pltpu.VMEM((rows, slots), jnp.bfloat16),
                pltpu.VMEM((rows, slots), jnp.bfloat16),
                pltpu.VMEM((rows, 1), jnp.float32),
                pltpu.VMEM((rows, 1), jnp.float32),
            ],
        ),
        out_shape=out_shape,
        cost_estimate=pl.CostEstimate(flops=4 * rows * slots * part, bytes_accessed=4 * slots * part, transcendentals=0),
        name="force_own" if own else "force",
    )(spot.reshape(1), put, own_rows, weights, s_slots, t_slots)


def grouped(student, teacher, bw_table, bw_index, group_ids, counts):
    ways = lax.axis_size("pair")
    pair = lax.axis_index("pair")
    rows, width = student.shape
    part = width // ways
    samples = rows * ways
    slots = GROUPS * SLOTS
    latent = float(width * lax.axis_size("value"))
    far_first = sorted(range(1, ways), key=lambda k: -k)
    chunks = CHUNKS if part % (CHUNKS * SLOTS) == 0 else 1
    size = part // chunks

    arrived = []
    for x in (student, teacher):
        for c in range(chunks):
            if len(arrived) >= FLIGHT:
                x, arrived[-FLIGHT] = lax.optimization_barrier((x, arrived[-FLIGHT]))
            arrived.append(exchange(x, pair, ways, c * size, size, far_first))
    student_k, teacher_k = arrived[:chunks], arrived[chunks:]

    same = group_ids[:, None] == group_ids[None, :]
    ids = jnp.arange(samples, dtype=jnp.int32)
    place = jnp.sum(same & (ids[None, :] < ids[:, None]), axis=1, dtype=jnp.int32)
    slot = group_ids * SLOTS + place
    slot_k = jnp.concatenate([lax.dynamic_slice_in_dim(slot, (pair ^ k) * rows, rows) for k in range(ways)])
    spots = jnp.arange(slots, dtype=jnp.int32)
    pick = (spots[:, None] == slot_k[None, :]).astype(jnp.bfloat16)
    put = (slot_k[:, None] == spots[None, :]).astype(jnp.bfloat16)

    def slotted(chunked):
        carry = None
        for c in range(chunks):
            carry = to_slots(pick, chunked[c], carry, c, chunks, part)
        return carry

    def gram(a, b):
        a, b = (x.reshape(GROUPS, SLOTS, part) for x in (a, b))
        return jnp.einsum("gsv,gtv->gst", a, b, preferred_element_type=jnp.float32)

    student_s = slotted(student_k)
    gram_self = all_sum(gram(student_s, student_s).reshape(slots, SLOTS)).reshape(GROUPS, SLOTS, SLOTS)
    teacher_s = slotted(teacher_k)
    t_wide = teacher.astype(jnp.float32)
    norm_own = jnp.sum(t_wide * t_wide, axis=1)
    norm_t = jnp.sum(jnp.where(spots[:, None] == slot_k[None, :rows], norm_own[None, :], 0.0), axis=1)
    norm_t = norm_t.reshape(GROUPS, 1, SLOTS)
    cross = jnp.concatenate(
        [gram(student_s, teacher_s), jnp.broadcast_to(norm_t, (GROUPS, PAD, SLOTS))], axis=1
    )
    cross = all_sum(cross.reshape(-1, SLOTS)).reshape(GROUPS, SLOTS + PAD, SLOTS)

    weights, loss = weights_of(gram_self, cross, counts, bw_table, bw_index, latent)
    loss = jnp.sum(loss[0]) / samples

    def force_to(k, spot=None):
        rows_k = jnp.concatenate([student_k[c][k] for c in range(chunks)], axis=1)
        return force_of(put[k * rows : (k + 1) * rows], rows_k, weights, student_s, teacher_s, ways, spot)

    sent = {k: swap(force_to(k).astype(jnp.float16), "pair", k) for k in far_first}
    out, reach = force_to(0, pair)
    for k in far_first:
        block = sent[k].astype(jnp.float32) * reach[:, :1]
        out = lax.dynamic_update_slice_in_dim(out, block, (pair ^ k) * part, 1)
    return (out, loss)


def per_device(student, teacher, bw_table, bw_index, group_ids):
    counts = jnp.sum(
        group_ids[None, :] == jnp.arange(GROUPS, dtype=jnp.int32)[:, None], axis=1, dtype=jnp.int32
    )
    args = (student, teacher, bw_table, bw_index, group_ids)
    force, loss = grouped(*args, counts)
    state = (jnp.max(counts) > SLOTS, force, loss)
    state = lax.while_loop(lambda s: s[0], lambda s: (jnp.zeros((), bool), *general(*args)), state)
    return state[1:]


def solution(mesh):
    placed_in = (P("pair", "value"), P("pair", "value"), P(), P(), P())
    return jax.shard_map(
        per_device, mesh=mesh, in_specs=placed_in, out_specs=(P("pair", "value"), P()), check_vma=False
    )
```

```python
import functools

import jax
import jax.numpy as jnp
from jax import lax
from jax.experimental import pallas as pl
from jax.experimental.pallas import tpu as pltpu
from jax.sharding import PartitionSpec as P

GROUPS = 16
SLOTS = 128
ROWS = 512
PAD = 16
HALF_TOP = 32768.0
FLIGHT = 4
CHUNKS = 4


def kernel_terms(
    gram_self, gram_cross, norm_rows, norm_student, norm_teacher, same_group, heights, latent
):
    dist_self = jnp.maximum(norm_rows[..., :, None] + norm_student[..., None, :] - 2.0 * gram_self, 0.0)
    dist_cross = jnp.maximum(norm_rows[..., :, None] + norm_teacher[..., None, :] - 2.0 * gram_cross, 0.0)
    kern_self = jnp.zeros_like(dist_self)
    kern_cross = jnp.zeros_like(dist_cross)
    weight_self = jnp.zeros_like(dist_self)
    weight_cross = jnp.zeros_like(dist_cross)
    count = heights.shape[0]
    for member in range(count):
        height = heights[member]
        width_now = height * latent
        exp_self = jnp.exp(-dist_self / width_now)
        exp_cross = jnp.exp(-dist_cross / width_now)
        kern_self = kern_self + exp_self
        kern_cross = kern_cross + exp_cross
        weight_self = weight_self + exp_self / height
        weight_cross = weight_cross + exp_cross / height
    kern_self = kern_self / count * same_group
    kern_cross = kern_cross / count * same_group
    weight_self = weight_self / count * same_group
    weight_cross = weight_cross / count * same_group
    row_loss = jnp.sum(kern_self - 2.0 * kern_cross, axis=-1)
    total_self = jnp.sum(weight_self, axis=-1)
    total_cross = jnp.sum(weight_cross, axis=-1)
    return (
        weight_self.astype(jnp.bfloat16),
        weight_cross.astype(jnp.bfloat16),
        row_loss,
        total_self,
        total_cross,
    )


def pick_heights(bw_table, bw_index):
    table_slots = jnp.arange(bw_table.shape[0], dtype=jnp.int32)
    return jnp.sum(
        jnp.where(bw_index[:, None] == table_slots[None, :], bw_table[None, :], 0.0), axis=1
    )


def swap(x, axis, bits):
    count = lax.axis_size(axis)
    return lax.ppermute(x, axis, [(i, i ^ bits) for i in range(count)])


def take(x, index):
    return lax.dynamic_index_in_dim(x, index, 0, keepdims=False)


def placed(parts, me):
    x = jnp.stack(parts)
    bit = 1
    while bit < len(parts):
        order = [i ^ bit for i in range(len(parts))]
        x = jnp.where((me & bit) != 0, jnp.stack([x[i] for i in order]), x)
        bit *= 2
    return x


def reduce_stages():
    values = lax.axis_size("value")
    value = lax.axis_index("value")
    pair = lax.axis_index("pair")
    stages = [("value", 1, min(values, 2), value & 1)]
    stages.append(("pair", 1, lax.axis_size("pair"), pair))
    if values >= 8:
        stages.append(("value", 2, 4, (value >> 1) & 3))
        done = 8
    else:
        done = 2
    rest = []
    while done < values:
        rest.append(done)
        done *= 2
    return stages, rest


def all_sum(x):
    return list(sum_steps([x]))[-1]


def sum_steps(held):
    x = held[0]
    stages, rest = reduce_stages()
    for axis, unit, ways, me in stages:
        x = x.reshape((ways, x.shape[0] // ways) + x.shape[1:])
        got = [swap(take(x, me ^ k), axis, unit * k) for k in range(1, ways)]
        held[0] = sum(got, take(x, me))
        yield held[0]
        x = held[0]
    for bits in rest:
        x = x + swap(x, "value", bits)
    for axis, unit, ways, me in reversed(stages):
        got = [x] + [swap(x, axis, unit * k) for k in range(1, ways)]
        x = placed(got, me)
        held[0] = x.reshape((x.shape[0] * x.shape[1],) + x.shape[2:])
        yield held[0]
        x = held[0]


def pieces_of(x, pair, ways, lo, size):
    part = x.shape[1] // ways
    return [lax.dynamic_slice_in_dim(x, (pair ^ k) * part + lo, size, 1) for k in range(ways)]


def exchange(x, pair, ways, lo, size, order):
    pieces = pieces_of(x, pair, ways, lo, size)
    got = {0: pieces[0]}
    for k in order:
        got[k] = swap(pieces[k], "pair", k)
    return [got[k] for k in range(ways)]


def general(student, teacher, bw_table, bw_index, group_ids):
    ways = lax.axis_size("pair")
    pair = lax.axis_index("pair")
    rows, width = student.shape
    part = width // ways
    samples = rows * ways
    latent = float(width * lax.axis_size("value"))
    order = list(range(1, ways))
    block = SLOTS

    def gathered(x):
        full = jnp.zeros((samples, part), x.dtype)
        for k, got in enumerate(exchange(x, pair, ways, 0, part, order)):
            full = lax.dynamic_update_slice_in_dim(full, got, (pair ^ k) * rows, 0)
        return full

    def lane_sum(x):
        flat = x.reshape(-1, SLOTS)
        padded = jnp.pad(flat, ((0, -flat.shape[0] % 256), (0, 0)))
        return all_sum(padded)[: flat.shape[0]].reshape(x.shape)

    student_all, teacher_all = gathered(student), gathered(teacher)
    norms = jnp.stack([jnp.sum(x.astype(jnp.float32) ** 2, axis=1) for x in (student_all, teacher_all)])
    norm_student, norm_teacher = lane_sum(norms)
    heights = pick_heights(bw_table, bw_index)
    dims = (((1,), (1,)), ((), ()))

    def step(b, state):
        force, loss = state
        own = lax.dynamic_slice_in_dim(student_all, b * block, block)
        grams = [
            lax.dot_general(own, x, dims, preferred_element_type=jnp.float32) for x in (student_all, teacher_all)
        ]
        gram_self, gram_cross = lane_sum(jnp.stack(grams))
        own_ids = lax.dynamic_slice_in_dim(group_ids, b * block, block)
        same_group = (own_ids[:, None] == group_ids[None, :]).astype(jnp.float32)
        group_sizes = jnp.sum(same_group, axis=1)
        norm_rows = lax.dynamic_slice_in_dim(norm_student, b * block, block)
        weight_self, weight_cross, row_loss, total_self, total_cross = kernel_terms(
            gram_self, gram_cross, norm_rows, norm_student, norm_teacher, same_group, heights, latent
        )
        pulled = own.astype(jnp.float32) * (total_cross - total_self)[:, None]
        pulled = pulled + jnp.dot(weight_self, student_all, preferred_element_type=jnp.float32)
        pulled = pulled - jnp.dot(weight_cross, teacher_all, preferred_element_type=jnp.float32)
        pulled = pulled / group_sizes[:, None]
        force = lax.dynamic_update_slice_in_dim(force, pulled, b * block, 0)
        return force, loss + jnp.sum(row_loss / group_sizes)

    start = (jnp.zeros((samples, part), jnp.float32), jnp.zeros((), jnp.float32))
    force, loss = lax.fori_loop(0, samples // block, step, start)
    force = force.reshape(ways, rows, part)
    out = jnp.zeros((rows, width), jnp.float32)
    for k in range(ways):
        sent = take(force, pair ^ k)
        sent = swap(sent, "pair", k) if k else sent
        out = lax.dynamic_update_slice_in_dim(out, sent, (pair ^ k) * part, 1)
    return (out, loss / samples)


def slot_kernel(ways, first, *refs):
    pick, refs = refs[0], refs[1:]
    blocks, refs = refs[:ways], refs[ways:]
    slots_out, held = refs if first else refs[1:]
    rows = blocks[0].shape[0]

    @pl.when(pl.program_id(0) == 0)
    def _():
        for k in range(ways):
            held[k * rows : (k + 1) * rows] = blocks[k][...]

    slots_out[...] = jnp.dot(pick[...], held[...], preferred_element_type=jnp.float32).astype(jnp.bfloat16)


def to_slots(pick, blocks, carry, chunk, chunks, part):
    ways = len(blocks)
    rows, size = blocks[0].shape
    slots = pick.shape[0]
    first = carry is None
    in_specs = [pl.BlockSpec((ROWS, ways * rows), lambda i: (i, 0))]
    in_specs += [pl.BlockSpec((rows, size), lambda i: (0, 0))] * ways
    args = [pick, *blocks]
    aliases = {}
    if not first:
        in_specs.append(pl.BlockSpec(memory_space=pl.ANY))
        aliases = {len(args): 0}
        args.append(carry)
    return pl.pallas_call(
        functools.partial(slot_kernel, ways, first),
        grid=(slots // ROWS,),
        in_specs=in_specs,
        out_specs=pl.BlockSpec((ROWS, size), lambda i: (i, chunk)),
        out_shape=jax.ShapeDtypeStruct((slots, part), jnp.bfloat16),
        scratch_shapes=[pltpu.VMEM((ways * rows, size), jnp.bfloat16)],
        input_output_aliases=aliases,
        cost_estimate=pl.CostEstimate(
            flops=2 * slots * size * ways * rows, bytes_accessed=slots * ways * rows * 2, transcendentals=0
        ),
        name="slots",
    )(*args)


def weight_kernel(latent, counts, index, table, self_ref, cross_ref, out, loss):
    step = pl.program_id(0)
    row = lax.broadcasted_iota(jnp.int32, (SLOTS, SLOTS), 0)
    col = lax.broadcasted_iota(jnp.int32, (SLOTS, SLOTS), 1)
    members = index.shape[0]
    scale = [-1.0 / (table[index[m]] * latent) for m in range(members)]
    inverse = [1.0 / (table[index[m]] * members) for m in range(members)]

    @pl.when(step == 0)
    def _():
        loss[...] = jnp.zeros_like(loss)

    for g in range(self_ref.shape[0]):
        size = counts[step * self_ref.shape[0] + g]
        used = (row < size) & (col < size)
        gram_self = self_ref[g]
        diag = jnp.where(row == col, gram_self, 0.0)
        norm_col = jnp.sum(diag, axis=0, keepdims=True)
        norm_row = jnp.sum(diag, axis=1, keepdims=True)

        def terms(gram, norm):
            both = norm_row + norm
            dist = jnp.maximum(both - 2.0 * gram, 0.0)
            kern = jnp.zeros_like(dist)
            weight = jnp.zeros_like(dist)
            for m in range(members):
                e = jnp.exp(dist * scale[m])
                kern = kern + e
                weight = weight + e * inverse[m]
            kern = jnp.where(used, kern, 0.0)
            weight = jnp.where(used, weight, 0.0)
            span = dist + both * (2.0 ** -10) + 1e-30
            return kern, weight, weight * (span * lax.rsqrt(span))

        kern_s, weight_s, reach_s = terms(gram_self, norm_col)
        kern_c, weight_c, reach_c = terms(cross_ref[g, :SLOTS], cross_ref[g, SLOTS : SLOTS + 1])
        count = jnp.maximum(size, 1).astype(jnp.float32)
        pull = jnp.sum(weight_c - weight_s, axis=1, keepdims=True)
        reach = jnp.sum(reach_s + reach_c, axis=1, keepdims=True) * (1.01 / count)
        reach = jnp.maximum(reach, 1e-30).astype(jnp.bfloat16).astype(jnp.float32)
        high = pull.astype(jnp.bfloat16).astype(jnp.float32)
        mid = (pull - high).astype(jnp.bfloat16).astype(jnp.float32)
        low = pull - high - mid
        extra = jnp.where(col == 0, high, jnp.where(col == 1, mid, jnp.where(col == 2, low, 0.0)))
        extra = jnp.where(col == 3, count, jnp.where(col == 4, reach, extra))
        at = slice(g * SLOTS, (g + 1) * SLOTS)
        out[at, :SLOTS] = weight_s.astype(jnp.bfloat16)
        out[at, SLOTS : 2 * SLOTS] = (-weight_c).astype(jnp.bfloat16)
        out[at, 2 * SLOTS :] = extra.astype(jnp.bfloat16)
        part = jnp.sum(kern_s - 2.0 * kern_c, axis=0, keepdims=True) * (1.0 / (count * members))
        loss[...] += jnp.broadcast_to(part, loss.shape)


def weights_of(gram_self, cross, counts, bw_table, bw_index, latent):
    smem = pl.BlockSpec(memory_space=pltpu.SMEM)
    high = cross.shape[1]
    held = 4
    return pl.pallas_call(
        functools.partial(weight_kernel, latent),
        grid=(GROUPS // held,),
        in_specs=[
            smem,
            smem,
            smem,
            pl.BlockSpec((held, SLOTS, SLOTS), lambda g: (g, 0, 0)),
            pl.BlockSpec((held, high, SLOTS), lambda g: (g, 0, 0)),
        ],
        out_specs=[
            pl.BlockSpec((held * SLOTS, 3 * SLOTS), lambda g: (g, 0)),
            pl.BlockSpec((8, SLOTS), lambda g: (0, 0)),
        ],
        out_shape=[
            jax.ShapeDtypeStruct((GROUPS * SLOTS, 3 * SLOTS), jnp.bfloat16),
            jax.ShapeDtypeStruct((8, SLOTS), jnp.float32),
        ],
        cost_estimate=pl.CostEstimate(flops=GROUPS * SLOTS * SLOTS * 60, bytes_accessed=4 << 20, transcendentals=0),
        name="weights",
    )(counts, bw_index, bw_table, gram_self, cross)


def force_kernel(own, spot, put, own_rows, weights, s_slots, t_slots, *refs):
    if own:
        out, reach_out, w_s, w_c, pull, scale = refs
    else:
        out, w_s, w_c, pull, scale = refs
    rows, slots = put.shape

    @pl.when(pl.program_id(0) == 0)
    def _():
        extra = jnp.zeros((rows, SLOTS), jnp.float32)
        for g in range(slots // SLOTS):
            at = slice(g * SLOTS, (g + 1) * SLOTS)
            found = jnp.dot(put[:, at], weights[at], preferred_element_type=jnp.float32)
            w_s[:, at] = found[:, :SLOTS].astype(jnp.bfloat16)
            w_c[:, at] = found[:, SLOTS : 2 * SLOTS].astype(jnp.bfloat16)
            extra = extra + found[:, 2 * SLOTS :]
        pull[...] = extra[:, 0:1] + extra[:, 1:2] + extra[:, 2:3]
        size = extra[:, 3:4]
        reach = extra[:, 4:5]
        if own:
            scale[...] = 1.0 / size
            reach_out[...] = jnp.broadcast_to(reach * (1.0 / HALF_TOP), reach_out.shape)
        else:
            scale[...] = HALF_TOP / (size * reach)

    force = own_rows[...].astype(jnp.float32) * pull[...]
    force = force + jnp.dot(w_s[...], s_slots[...], preferred_element_type=jnp.float32)
    force = force + jnp.dot(w_c[...], t_slots[...], preferred_element_type=jnp.float32)
    out[...] = force * scale[...]


def force_of(put, own_rows, weights, s_slots, t_slots, ways, spot=None):
    own = spot is not None
    rows = put.shape[0]
    slots, part = s_slots.shape
    size = min(part, 512)
    steps = part // size
    full = lambda shape: pl.BlockSpec(shape, lambda c, spot: (0, 0))
    cols = lambda high: pl.BlockSpec((high, size), lambda c, spot: (0, c))
    if own:
        out_specs = [
            pl.BlockSpec((rows, size), lambda c, spot: (0, spot[0] * steps + c)),
            full((rows, SLOTS)),
        ]
        out_shape = [
            jax.ShapeDtypeStruct((rows, part * ways), jnp.float32),
            jax.ShapeDtypeStruct((rows, SLOTS), jnp.float32),
        ]
    else:
        out_specs = cols(rows)
        out_shape = jax.ShapeDtypeStruct((rows, part), jnp.float32)
        spot = jnp.zeros((), jnp.int32)
    return pl.pallas_call(
        functools.partial(force_kernel, own),
        grid_spec=pltpu.PrefetchScalarGridSpec(
            num_scalar_prefetch=1,
            grid=(steps,),
            in_specs=[full((rows, slots)), cols(rows), full(weights.shape), cols(slots), cols(slots)],
            out_specs=out_specs,
            scratch_shapes=[
                pltpu.VMEM((rows, slots), jnp.bfloat16),
                pltpu.VMEM((rows, slots), jnp.bfloat16),
                pltpu.VMEM((rows, 1), jnp.float32),
                pltpu.VMEM((rows, 1), jnp.float32),
            ],
        ),
        out_shape=out_shape,
        cost_estimate=pl.CostEstimate(flops=4 * rows * slots * part, bytes_accessed=4 * slots * part, transcendentals=0),
        name="force_own" if own else "force",
    )(spot.reshape(1), put, own_rows, weights, s_slots, t_slots)


def grouped(student, teacher, bw_table, bw_index, group_ids, counts):
    ways = lax.axis_size("pair")
    pair = lax.axis_index("pair")
    rows, width = student.shape
    part = width // ways
    samples = rows * ways
    slots = GROUPS * SLOTS
    latent = float(width * lax.axis_size("value"))
    far_first = sorted(range(1, ways), key=lambda k: -k)
    chunks = CHUNKS if part % (CHUNKS * SLOTS) == 0 else 1
    size = part // chunks

    arrived = []
    for x in (student, teacher):
        for c in range(chunks):
            if len(arrived) >= FLIGHT:
                x, arrived[-FLIGHT] = lax.optimization_barrier((x, arrived[-FLIGHT]))
            arrived.append(exchange(x, pair, ways, c * size, size, far_first))
    student_k, teacher_k = arrived[:chunks], arrived[chunks:]

    same = group_ids[:, None] == group_ids[None, :]
    ids = jnp.arange(samples, dtype=jnp.int32)
    place = jnp.sum(same & (ids[None, :] < ids[:, None]), axis=1, dtype=jnp.int32)
    slot = group_ids * SLOTS + place
    slot_k = jnp.concatenate([lax.dynamic_slice_in_dim(slot, (pair ^ k) * rows, rows) for k in range(ways)])
    spots = jnp.arange(slots, dtype=jnp.int32)
    pick = (spots[:, None] == slot_k[None, :]).astype(jnp.bfloat16)
    put = (slot_k[:, None] == spots[None, :]).astype(jnp.bfloat16)

    def slotted(chunked):
        carry = None
        for c in range(chunks):
            carry = to_slots(pick, chunked[c], carry, c, chunks, part)
        return carry

    def gram(a, b):
        a, b = (x.reshape(GROUPS, SLOTS, part) for x in (a, b))
        return jnp.einsum("gsv,gtv->gst", a, b, preferred_element_type=jnp.float32)

    student_s = slotted(student_k)
    held = [gram(student_s, student_s).reshape(slots, SLOTS)]
    steps = sum_steps(held)
    for c in range(max(chunks - 2, 1), chunks):
        next(steps)
        held[0], teacher_k[c] = lax.optimization_barrier((held[0], teacher_k[c]))
    teacher_s = slotted(teacher_k)
    next(steps)
    held[0], teacher_s = lax.optimization_barrier((held[0], teacher_s))
    gram_self = list(steps)[-1].reshape(GROUPS, SLOTS, SLOTS)
    t_wide = teacher.astype(jnp.float32)
    norm_own = jnp.sum(t_wide * t_wide, axis=1)
    norm_t = jnp.sum(jnp.where(spots[:, None] == slot_k[None, :rows], norm_own[None, :], 0.0), axis=1)
    norm_t = norm_t.reshape(GROUPS, 1, SLOTS)
    cross = jnp.concatenate(
        [gram(student_s, teacher_s), jnp.broadcast_to(norm_t, (GROUPS, PAD, SLOTS))], axis=1
    )
    cross = all_sum(cross.reshape(-1, SLOTS)).reshape(GROUPS, SLOTS + PAD, SLOTS)

    weights, loss = weights_of(gram_self, cross, counts, bw_table, bw_index, latent)
    loss = jnp.sum(loss[0]) / samples

    def force_to(k, spot=None):
        rows_k = jnp.concatenate([student_k[c][k] for c in range(chunks)], axis=1)
        return force_of(put[k * rows : (k + 1) * rows], rows_k, weights, student_s, teacher_s, ways, spot)

    sent = {k: swap(force_to(k).astype(jnp.float16), "pair", k) for k in far_first}
    out, reach = force_to(0, pair)
    for k in far_first:
        block = sent[k].astype(jnp.float32) * reach[:, :1]
        out = lax.dynamic_update_slice_in_dim(out, block, (pair ^ k) * part, 1)
    return (out, loss)


def per_device(student, teacher, bw_table, bw_index, group_ids):
    counts = jnp.sum(
        group_ids[None, :] == jnp.arange(GROUPS, dtype=jnp.int32)[:, None], axis=1, dtype=jnp.int32
    )
    args = (student, teacher, bw_table, bw_index, group_ids)
    force, loss = grouped(*args, counts)
    state = (jnp.max(counts) > SLOTS, force, loss)
    state = lax.while_loop(lambda s: s[0], lambda s: (jnp.zeros((), bool), *general(*args)), state)
    return state[1:]


def solution(mesh):
    placed_in = (P("pair", "value"), P("pair", "value"), P(), P(), P())
    return jax.shard_map(
        per_device, mesh=mesh, in_specs=placed_in, out_specs=(P("pair", "value"), P()), check_vma=False
    )
```

```python
import functools

import jax
import jax.numpy as jnp
from jax import lax
from jax.experimental import pallas as pl
from jax.experimental.pallas import tpu as pltpu
from jax.sharding import PartitionSpec as P

GROUPS = 16
SLOTS = 128
ROWS = 512
PAD = 16
HALF_TOP = 32768.0
FLIGHT = 4
CHUNKS = 4


def kernel_terms(
    gram_self, gram_cross, norm_rows, norm_student, norm_teacher, same_group, heights, latent
):
    dist_self = jnp.maximum(norm_rows[..., :, None] + norm_student[..., None, :] - 2.0 * gram_self, 0.0)
    dist_cross = jnp.maximum(norm_rows[..., :, None] + norm_teacher[..., None, :] - 2.0 * gram_cross, 0.0)
    kern_self = jnp.zeros_like(dist_self)
    kern_cross = jnp.zeros_like(dist_cross)
    weight_self = jnp.zeros_like(dist_self)
    weight_cross = jnp.zeros_like(dist_cross)
    count = heights.shape[0]
    for member in range(count):
        height = heights[member]
        width_now = height * latent
        exp_self = jnp.exp(-dist_self / width_now)
        exp_cross = jnp.exp(-dist_cross / width_now)
        kern_self = kern_self + exp_self
        kern_cross = kern_cross + exp_cross
        weight_self = weight_self + exp_self / height
        weight_cross = weight_cross + exp_cross / height
    kern_self = kern_self / count * same_group
    kern_cross = kern_cross / count * same_group
    weight_self = weight_self / count * same_group
    weight_cross = weight_cross / count * same_group
    row_loss = jnp.sum(kern_self - 2.0 * kern_cross, axis=-1)
    total_self = jnp.sum(weight_self, axis=-1)
    total_cross = jnp.sum(weight_cross, axis=-1)
    return (
        weight_self.astype(jnp.bfloat16),
        weight_cross.astype(jnp.bfloat16),
        row_loss,
        total_self,
        total_cross,
    )


def pick_heights(bw_table, bw_index):
    table_slots = jnp.arange(bw_table.shape[0], dtype=jnp.int32)
    return jnp.sum(
        jnp.where(bw_index[:, None] == table_slots[None, :], bw_table[None, :], 0.0), axis=1
    )


def swap(x, axis, bits):
    count = lax.axis_size(axis)
    return lax.ppermute(x, axis, [(i, i ^ bits) for i in range(count)])


def take(x, index):
    return lax.dynamic_index_in_dim(x, index, 0, keepdims=False)


def placed(parts, me):
    x = jnp.stack(parts)
    bit = 1
    while bit < len(parts):
        order = [i ^ bit for i in range(len(parts))]
        x = jnp.where((me & bit) != 0, jnp.stack([x[i] for i in order]), x)
        bit *= 2
    return x


def reduce_stages():
    values = lax.axis_size("value")
    value = lax.axis_index("value")
    pair = lax.axis_index("pair")
    stages = [("value", 1, min(values, 2), value & 1)]
    stages.append(("pair", 1, lax.axis_size("pair"), pair))
    if values >= 8:
        stages.append(("value", 2, 4, (value >> 1) & 3))
        done = 8
    else:
        done = 2
    rest = []
    while done < values:
        rest.append(done)
        done *= 2
    return stages, rest


def all_sum(x):
    stages, rest = reduce_stages()
    for axis, unit, ways, me in stages:
        x = x.reshape((ways, x.shape[0] // ways) + x.shape[1:])
        got = [swap(take(x, me ^ k), axis, unit * k) for k in range(1, ways)]
        x = sum(got, take(x, me))
    for bits in rest:
        x = x + swap(x, "value", bits)
    for axis, unit, ways, me in reversed(stages):
        got = [x] + [swap(x, axis, unit * k) for k in range(1, ways)]
        x = placed(got, me)
        x = x.reshape((x.shape[0] * x.shape[1],) + x.shape[2:])
    return x


def pieces_of(x, pair, ways, lo, size):
    part = x.shape[1] // ways
    return [lax.dynamic_slice_in_dim(x, (pair ^ k) * part + lo, size, 1) for k in range(ways)]


def exchange(x, pair, ways, lo, size, order):
    pieces = pieces_of(x, pair, ways, lo, size)
    got = {0: pieces[0]}
    for k in order:
        got[k] = swap(pieces[k], "pair", k)
    return [got[k] for k in range(ways)]


def general(student, teacher, bw_table, bw_index, group_ids):
    ways = lax.axis_size("pair")
    pair = lax.axis_index("pair")
    rows, width = student.shape
    part = width // ways
    samples = rows * ways
    latent = float(width * lax.axis_size("value"))
    order = list(range(1, ways))
    block = SLOTS

    def gathered(x):
        full = jnp.zeros((samples, part), x.dtype)
        for k, got in enumerate(exchange(x, pair, ways, 0, part, order)):
            full = lax.dynamic_update_slice_in_dim(full, got, (pair ^ k) * rows, 0)
        return full

    def lane_sum(x):
        flat = x.reshape(-1, SLOTS)
        padded = jnp.pad(flat, ((0, -flat.shape[0] % 256), (0, 0)))
        return all_sum(padded)[: flat.shape[0]].reshape(x.shape)

    student_all, teacher_all = gathered(student), gathered(teacher)
    norms = jnp.stack([jnp.sum(x.astype(jnp.float32) ** 2, axis=1) for x in (student_all, teacher_all)])
    norm_student, norm_teacher = lane_sum(norms)
    heights = pick_heights(bw_table, bw_index)
    dims = (((1,), (1,)), ((), ()))

    def step(b, state):
        force, loss = state
        own = lax.dynamic_slice_in_dim(student_all, b * block, block)
        grams = [
            lax.dot_general(own, x, dims, preferred_element_type=jnp.float32) for x in (student_all, teacher_all)
        ]
        gram_self, gram_cross = lane_sum(jnp.stack(grams))
        own_ids = lax.dynamic_slice_in_dim(group_ids, b * block, block)
        same_group = (own_ids[:, None] == group_ids[None, :]).astype(jnp.float32)
        group_sizes = jnp.sum(same_group, axis=1)
        norm_rows = lax.dynamic_slice_in_dim(norm_student, b * block, block)
        weight_self, weight_cross, row_loss, total_self, total_cross = kernel_terms(
            gram_self, gram_cross, norm_rows, norm_student, norm_teacher, same_group, heights, latent
        )
        pulled = own.astype(jnp.float32) * (total_cross - total_self)[:, None]
        pulled = pulled + jnp.dot(weight_self, student_all, preferred_element_type=jnp.float32)
        pulled = pulled - jnp.dot(weight_cross, teacher_all, preferred_element_type=jnp.float32)
        pulled = pulled / group_sizes[:, None]
        force = lax.dynamic_update_slice_in_dim(force, pulled, b * block, 0)
        return force, loss + jnp.sum(row_loss / group_sizes)

    start = (jnp.zeros((samples, part), jnp.float32), jnp.zeros((), jnp.float32))
    force, loss = lax.fori_loop(0, samples // block, step, start)
    force = force.reshape(ways, rows, part)
    out = jnp.zeros((rows, width), jnp.float32)
    for k in range(ways):
        sent = take(force, pair ^ k)
        sent = swap(sent, "pair", k) if k else sent
        out = lax.dynamic_update_slice_in_dim(out, sent, (pair ^ k) * part, 1)
    return (out, loss / samples)


def slot_kernel(ways, first, *refs):
    pick, refs = refs[0], refs[1:]
    blocks, refs = refs[:ways], refs[ways:]
    slots_out, held = refs if first else refs[1:]
    rows = blocks[0].shape[0]

    @pl.when(pl.program_id(0) == 0)
    def _():
        for k in range(ways):
            held[k * rows : (k + 1) * rows] = blocks[k][...]

    slots_out[...] = jnp.dot(pick[...], held[...], preferred_element_type=jnp.float32).astype(jnp.bfloat16)


def to_slots(pick, blocks, carry, chunk, chunks, part):
    ways = len(blocks)
    rows, size = blocks[0].shape
    slots = pick.shape[0]
    first = carry is None
    in_specs = [pl.BlockSpec((ROWS, ways * rows), lambda i: (i, 0))]
    in_specs += [pl.BlockSpec((rows, size), lambda i: (0, 0))] * ways
    args = [pick, *blocks]
    aliases = {}
    if not first:
        in_specs.append(pl.BlockSpec(memory_space=pl.ANY))
        aliases = {len(args): 0}
        args.append(carry)
    return pl.pallas_call(
        functools.partial(slot_kernel, ways, first),
        grid=(slots // ROWS,),
        in_specs=in_specs,
        out_specs=pl.BlockSpec((ROWS, size), lambda i: (i, chunk)),
        out_shape=jax.ShapeDtypeStruct((slots, part), jnp.bfloat16),
        scratch_shapes=[pltpu.VMEM((ways * rows, size), jnp.bfloat16)],
        input_output_aliases=aliases,
        cost_estimate=pl.CostEstimate(
            flops=2 * slots * size * ways * rows, bytes_accessed=slots * ways * rows * 2, transcendentals=0
        ),
        name="slots",
    )(*args)


def weight_kernel(latent, counts, index, table, self_ref, cross_ref, out, loss):
    step = pl.program_id(0)
    row = lax.broadcasted_iota(jnp.int32, (SLOTS, SLOTS), 0)
    col = lax.broadcasted_iota(jnp.int32, (SLOTS, SLOTS), 1)
    members = index.shape[0]
    scale = [-1.0 / (table[index[m]] * latent) for m in range(members)]
    inverse = [1.0 / (table[index[m]] * members) for m in range(members)]

    @pl.when(step == 0)
    def _():
        loss[...] = jnp.zeros_like(loss)

    for g in range(self_ref.shape[0]):
        size = counts[step * self_ref.shape[0] + g]
        used = (row < size) & (col < size)
        gram_self = self_ref[g]
        diag = jnp.where(row == col, gram_self, 0.0)
        norm_col = jnp.sum(diag, axis=0, keepdims=True)
        norm_row = jnp.sum(diag, axis=1, keepdims=True)

        def terms(gram, norm):
            both = norm_row + norm
            dist = jnp.maximum(both - 2.0 * gram, 0.0)
            kern = jnp.zeros_like(dist)
            weight = jnp.zeros_like(dist)
            for m in range(members):
                e = jnp.exp(dist * scale[m])
                kern = kern + e
                weight = weight + e * inverse[m]
            kern = jnp.where(used, kern, 0.0)
            weight = jnp.where(used, weight, 0.0)
            span = dist + both * (2.0 ** -10) + 1e-30
            return kern, weight, weight * (span * lax.rsqrt(span))

        kern_s, weight_s, reach_s = terms(gram_self, norm_col)
        kern_c, weight_c, reach_c = terms(cross_ref[g, :SLOTS], cross_ref[g, SLOTS : SLOTS + 1])
        count = jnp.maximum(size, 1).astype(jnp.float32)
        pull = jnp.sum(weight_c - weight_s, axis=1, keepdims=True)
        reach = jnp.sum(reach_s + reach_c, axis=1, keepdims=True) * (1.01 / count)
        reach = jnp.maximum(reach, 1e-30).astype(jnp.bfloat16).astype(jnp.float32)
        high = pull.astype(jnp.bfloat16).astype(jnp.float32)
        mid = (pull - high).astype(jnp.bfloat16).astype(jnp.float32)
        low = pull - high - mid
        extra = jnp.where(col == 0, high, jnp.where(col == 1, mid, jnp.where(col == 2, low, 0.0)))
        extra = jnp.where(col == 3, count, jnp.where(col == 4, reach, extra))
        at = slice(g * SLOTS, (g + 1) * SLOTS)
        out[at, :SLOTS] = weight_s.astype(jnp.bfloat16)
        out[at, SLOTS : 2 * SLOTS] = (-weight_c).astype(jnp.bfloat16)
        out[at, 2 * SLOTS :] = extra.astype(jnp.bfloat16)
        part = jnp.sum(kern_s - 2.0 * kern_c, axis=0, keepdims=True) * (1.0 / (count * members))
        loss[...] += jnp.broadcast_to(part, loss.shape)


def weights_of(gram_self, cross, counts, bw_table, bw_index, latent):
    smem = pl.BlockSpec(memory_space=pltpu.SMEM)
    high = cross.shape[1]
    held = 4
    return pl.pallas_call(
        functools.partial(weight_kernel, latent),
        grid=(GROUPS // held,),
        in_specs=[
            smem,
            smem,
            smem,
            pl.BlockSpec((held, SLOTS, SLOTS), lambda g: (g, 0, 0)),
            pl.BlockSpec((held, high, SLOTS), lambda g: (g, 0, 0)),
        ],
        out_specs=[
            pl.BlockSpec((held * SLOTS, 3 * SLOTS), lambda g: (g, 0)),
            pl.BlockSpec((8, SLOTS), lambda g: (0, 0)),
        ],
        out_shape=[
            jax.ShapeDtypeStruct((GROUPS * SLOTS, 3 * SLOTS), jnp.bfloat16),
            jax.ShapeDtypeStruct((8, SLOTS), jnp.float32),
        ],
        cost_estimate=pl.CostEstimate(flops=GROUPS * SLOTS * SLOTS * 60, bytes_accessed=4 << 20, transcendentals=0),
        name="weights",
    )(counts, bw_index, bw_table, gram_self, cross)


def force_kernel(own, steps, spot, put, weights, s_slots, t_slots, *refs):
    own_rows, refs = refs[:steps], refs[steps:]
    if own:
        out, reach_out, w_s, w_c, pull, scale = refs
    else:
        out, w_s, w_c, pull, scale = refs
    rows, slots = put.shape

    @pl.when(pl.program_id(0) == 0)
    def _():
        extra = jnp.zeros((rows, SLOTS), jnp.float32)
        for g in range(slots // SLOTS):
            at = slice(g * SLOTS, (g + 1) * SLOTS)
            found = jnp.dot(put[:, at], weights[at], preferred_element_type=jnp.float32)
            w_s[:, at] = found[:, :SLOTS].astype(jnp.bfloat16)
            w_c[:, at] = found[:, SLOTS : 2 * SLOTS].astype(jnp.bfloat16)
            extra = extra + found[:, 2 * SLOTS :]
        pull[...] = extra[:, 0:1] + extra[:, 1:2] + extra[:, 2:3]
        size = extra[:, 3:4]
        reach = extra[:, 4:5]
        if own:
            scale[...] = 1.0 / size
            reach_out[...] = jnp.broadcast_to(reach * (1.0 / HALF_TOP), reach_out.shape)
        else:
            scale[...] = HALF_TOP / (size * reach)

    force = jnp.dot(w_s[...], s_slots[...], preferred_element_type=jnp.float32)
    force = force + jnp.dot(w_c[...], t_slots[...], preferred_element_type=jnp.float32)
    for c in range(steps):

        @pl.when(pl.program_id(0) == c)
        def _():
            out[...] = (force + own_rows[c][...].astype(jnp.float32) * pull[...]) * scale[...]


def force_of(put, own_rows, weights, s_slots, t_slots, ways, spot=None):
    own = spot is not None
    rows = put.shape[0]
    slots, part = s_slots.shape
    steps = len(own_rows)
    size = part // steps
    full = lambda shape: pl.BlockSpec(shape, lambda c, spot: (0, 0))
    cols = lambda high: pl.BlockSpec((high, size), lambda c, spot: (0, c))
    if own:
        out_specs = [
            pl.BlockSpec((rows, size), lambda c, spot: (0, spot[0] * steps + c)),
            full((rows, SLOTS)),
        ]
        out_shape = [
            jax.ShapeDtypeStruct((rows, part * ways), jnp.float32),
            jax.ShapeDtypeStruct((rows, SLOTS), jnp.float32),
        ]
    else:
        out_specs = cols(rows)
        out_shape = jax.ShapeDtypeStruct((rows, part), jnp.float32)
        spot = jnp.zeros((), jnp.int32)
    return pl.pallas_call(
        functools.partial(force_kernel, own, steps),
        grid_spec=pltpu.PrefetchScalarGridSpec(
            num_scalar_prefetch=1,
            grid=(steps,),
            in_specs=[full((rows, slots)), full(weights.shape), cols(slots), cols(slots)] + [full((rows, size))] * steps,
            out_specs=out_specs,
            scratch_shapes=[
                pltpu.VMEM((rows, slots), jnp.bfloat16),
                pltpu.VMEM((rows, slots), jnp.bfloat16),
                pltpu.VMEM((rows, 1), jnp.float32),
                pltpu.VMEM((rows, 1), jnp.float32),
            ],
        ),
        out_shape=out_shape,
        cost_estimate=pl.CostEstimate(flops=4 * rows * slots * part, bytes_accessed=4 * slots * part, transcendentals=0),
        name="force_own" if own else "force",
    )(spot.reshape(1), put, weights, s_slots, t_slots, *own_rows)


def grouped(student, teacher, bw_table, bw_index, group_ids, counts):
    ways = lax.axis_size("pair")
    pair = lax.axis_index("pair")
    rows, width = student.shape
    part = width // ways
    samples = rows * ways
    slots = GROUPS * SLOTS
    latent = float(width * lax.axis_size("value"))
    far_first = sorted(range(1, ways), key=lambda k: -k)
    chunks = CHUNKS if part % (CHUNKS * SLOTS) == 0 else 1
    size = part // chunks

    arrived = []
    for x in (student, teacher):
        for c in range(chunks):
            if len(arrived) >= FLIGHT:
                x, arrived[-FLIGHT] = lax.optimization_barrier((x, arrived[-FLIGHT]))
            arrived.append(exchange(x, pair, ways, c * size, size, far_first))
    student_k, teacher_k = arrived[:chunks], arrived[chunks:]

    same = group_ids[:, None] == group_ids[None, :]
    ids = jnp.arange(samples, dtype=jnp.int32)
    place = jnp.sum(same & (ids[None, :] < ids[:, None]), axis=1, dtype=jnp.int32)
    slot = group_ids * SLOTS + place
    slot_k = jnp.concatenate([lax.dynamic_slice_in_dim(slot, (pair ^ k) * rows, rows) for k in range(ways)])
    spots = jnp.arange(slots, dtype=jnp.int32)
    pick = (spots[:, None] == slot_k[None, :]).astype(jnp.bfloat16)
    put = (slot_k[:, None] == spots[None, :]).astype(jnp.bfloat16)

    def slotted(chunked):
        carry = None
        for c in range(chunks):
            carry = to_slots(pick, chunked[c], carry, c, chunks, part)
        return carry

    def gram(a, b):
        a, b = (x.reshape(GROUPS, SLOTS, part) for x in (a, b))
        return jnp.einsum("gsv,gtv->gst", a, b, preferred_element_type=jnp.float32)

    student_s = slotted(student_k)
    gram_self = all_sum(gram(student_s, student_s).reshape(slots, SLOTS)).reshape(GROUPS, SLOTS, SLOTS)
    teacher_s = slotted(teacher_k)
    t_wide = teacher.astype(jnp.float32)
    norm_own = jnp.sum(t_wide * t_wide, axis=1)
    norm_t = jnp.sum(jnp.where(spots[:, None] == slot_k[None, :rows], norm_own[None, :], 0.0), axis=1)
    norm_t = norm_t.reshape(GROUPS, 1, SLOTS)
    cross = jnp.concatenate(
        [gram(student_s, teacher_s), jnp.broadcast_to(norm_t, (GROUPS, PAD, SLOTS))], axis=1
    )
    cross = all_sum(cross.reshape(-1, SLOTS)).reshape(GROUPS, SLOTS + PAD, SLOTS)

    weights, loss = weights_of(gram_self, cross, counts, bw_table, bw_index, latent)
    loss = jnp.sum(loss[0]) / samples

    def force_to(k, spot=None):
        rows_k = [student_k[c][k] for c in range(chunks)]
        return force_of(put[k * rows : (k + 1) * rows], rows_k, weights, student_s, teacher_s, ways, spot)

    sent = {k: swap(force_to(k).astype(jnp.float16), "pair", k) for k in far_first}
    out, reach = force_to(0, pair)
    for k in far_first:
        block = sent[k].astype(jnp.float32) * reach[:, :1]
        out = lax.dynamic_update_slice_in_dim(out, block, (pair ^ k) * part, 1)
    return (out, loss)


def per_device(student, teacher, bw_table, bw_index, group_ids):
    counts = jnp.sum(
        group_ids[None, :] == jnp.arange(GROUPS, dtype=jnp.int32)[:, None], axis=1, dtype=jnp.int32
    )
    args = (student, teacher, bw_table, bw_index, group_ids)
    force, loss = grouped(*args, counts)
    state = (jnp.max(counts) > SLOTS, force, loss)
    state = lax.while_loop(lambda s: s[0], lambda s: (jnp.zeros((), bool), *general(*args)), state)
    return state[1:]


def solution(mesh):
    placed_in = (P("pair", "value"), P("pair", "value"), P(), P(), P())
    return jax.shard_map(
        per_device, mesh=mesh, in_specs=placed_in, out_specs=(P("pair", "value"), P()), check_vma=False
    )
```
